64 devices in a mesh: dp: 4 (over x, y), ep: 16 (over z, core).
Axes of the slice: x: 2, y: 2, z: 8, core: 2. Of those that a mesh axis runs over, the one named last changes fastest.
The devices are a block of a 4x4x8 slice.
Arguments:
- hidden: bfloat16 [16384, 2048], P(('dp', 'ep')), parts along dimension 0
- norm_gain: float32 [2048], replicated
- router_w: bfloat16 [2048, 64], replicated
- topk_idx: int32 [16384, 6], P(('dp', 'ep')), parts along dimension 0
- w_gate: bfloat16 [64, 2048, 1408], P('ep')
- w_up: bfloat16 [64, 2048, 1408], P('ep')
- w_down: bfloat16 [64, 1408, 2048], P('ep')
- shared_gate: bfloat16 [2048, 2816], replicated
- shared_up: bfloat16 [2048, 2816], replicated
- shared_down: bfloat16 [2816, 2048], replicated
Outputs:
- output: bfloat16 [16384, 2048], P(('dp', 'ep')), parts along dimension 0
There are 4 independent parts. The reference program is written for one: setup_inputs(seed, part) draws one part's arguments, and reference() takes and returns one part's arrays. A program takes and returns all parts, laid end to end along the dimension named above; an argument that names none is the same for every part.
All inputs are finite; a program needn't handle non-finite values.
Results may differ from the reference program's by a relative error of at most 0.00127.
Values are sent between devices in bfloat16 or wider.
A program may use at most 768 MiB of HBM per device.

```python
import jax
import jax.numpy as jnp
from jax import lax

HIDDEN = 2048
EXPERTS = 64
TOP_K = 6
EXPERT_FF = 1408
SHARED_FF = 2816
GROUP_SIZE = 16
TOKENS = 256
ROW_BLOCK = 128
NORM_EPS = 1e-6

NUM_TOKENS = GROUP_SIZE * TOKENS
ROUTE_ROWS = NUM_TOKENS * TOP_K
NUM_BLOCKS = (ROUTE_ROWS + EXPERTS * (ROW_BLOCK - 1) + ROW_BLOCK - 1) // ROW_BLOCK


def draw_routing(route_key):
    mean_rows = TOKENS * TOP_K // EXPERTS
    half_rows = mean_rows // 2

    def one_device(dev_key):
        key_pair, key_shift, key_layout, key_tokens = jax.random.split(dev_key, 4)
        pair_perm = jax.random.permutation(key_pair, EXPERTS)
        shift_rows = jax.random.randint(key_shift, (EXPERTS // 2,), -half_rows, half_rows + 1)
        shift_rows = shift_rows.at[0].set(half_rows)
        pair_counts = jnp.stack([mean_rows + shift_rows, mean_rows - shift_rows], axis=1).reshape(EXPERTS)
        counts = jnp.zeros((EXPERTS,), jnp.int32).at[pair_perm].set(pair_counts)
        layout_order = jax.random.permutation(key_layout, EXPERTS)
        bounds = jnp.cumsum(counts[layout_order])
        positions = jnp.arange(TOKENS * TOP_K)
        range_index = jnp.sum(positions[:, None] >= bounds[None, :], axis=1)
        expert_grid = layout_order[range_index].reshape(TOP_K, TOKENS)
        token_perm = jax.random.permutation(key_tokens, TOKENS)
        return jnp.zeros((TOKENS, TOP_K), jnp.int32).at[token_perm].set(expert_grid.T)

    dev_keys = jax.random.split(route_key, GROUP_SIZE)
    return jax.vmap(one_device)(dev_keys).reshape(NUM_TOKENS, TOP_K).astype(jnp.int32)


def setup_inputs(seed: int = 0, part: int = 0) -> dict:
    base_key = jax.random.key(seed)
    part_key = jax.random.fold_in(base_key, part)
    key_hidden, key_route = jax.random.split(part_key, 2)
    weight_keys = jax.random.split(base_key, 8)
    in_scale = HIDDEN ** -0.5
    down_scale = (EXPERTS / TOP_K) * EXPERT_FF ** -0.5
    hidden = 0.5 * jax.random.normal(key_hidden, (NUM_TOKENS, HIDDEN), jnp.float32)
    norm_gain = jax.random.uniform(weight_keys[0], (HIDDEN,), jnp.float32, 0.5, 1.5)
    router_w = in_scale * jax.random.normal(weight_keys[1], (HIDDEN, EXPERTS), jnp.float32)
    w_gate = in_scale * jax.random.normal(weight_keys[2], (EXPERTS, HIDDEN, EXPERT_FF), jnp.float32)
    w_up = in_scale * jax.random.normal(weight_keys[3], (EXPERTS, HIDDEN, EXPERT_FF), jnp.float32)
    w_down = down_scale * jax.random.normal(weight_keys[4], (EXPERTS, EXPERT_FF, HIDDEN), jnp.float32)
    shared_gate = in_scale * jax.random.normal(weight_keys[5], (HIDDEN, SHARED_FF), jnp.float32)
    shared_up = in_scale * jax.random.normal(weight_keys[6], (HIDDEN, SHARED_FF), jnp.float32)
    shared_down = 0.5 * SHARED_FF ** -0.5 * jax.random.normal(weight_keys[7], (SHARED_FF, HIDDEN), jnp.float32)
    return {
        'hidden': hidden.astype(jnp.bfloat16),
        'norm_gain': norm_gain,
        'router_w': router_w.astype(jnp.bfloat16),
        'topk_idx': draw_routing(key_route),
        'w_gate': w_gate.astype(jnp.bfloat16),
        'w_up': w_up.astype(jnp.bfloat16),
        'w_down': w_down.astype(jnp.bfloat16),
        'shared_gate': shared_gate.astype(jnp.bfloat16),
        'shared_up': shared_up.astype(jnp.bfloat16),
        'shared_down': shared_down.astype(jnp.bfloat16),
    }


def rms_norm(hidden, norm_gain):
    hidden_f32 = hidden.astype(jnp.float32)
    inv_rms = lax.rsqrt(jnp.mean(hidden_f32 * hidden_f32, axis=-1, keepdims=True) + NORM_EPS)
    return (hidden_f32 * inv_rms * norm_gain).astype(jnp.bfloat16)


def swiglu_rows(rows_in, gate_w, up_w, down_w):
    gate_out = jnp.dot(rows_in, gate_w, preferred_element_type=jnp.float32)
    up_out = jnp.dot(rows_in, up_w, preferred_element_type=jnp.float32)
    activated = (jax.nn.silu(gate_out) * up_out).astype(jnp.bfloat16)
    return jnp.dot(activated, down_w, preferred_element_type=jnp.float32)


def reference(hidden, norm_gain, router_w, topk_idx, w_gate, w_up, w_down, shared_gate, shared_up, shared_down):
    normed = rms_norm(hidden, norm_gain)
    logits = jnp.dot(normed, router_w, preferred_element_type=jnp.float32)
    route_w = jnp.take_along_axis(jax.nn.softmax(logits, axis=-1), topk_idx, axis=1)
    shared_out = swiglu_rows(normed, shared_gate, shared_up, shared_down)
    flat_expert = topk_idx.reshape(-1)
    row_order = jnp.argsort(flat_expert, stable=True)
    sorted_expert = flat_expert[row_order]
    counts = jnp.zeros((EXPERTS,), jnp.int32).at[flat_expert].add(1)
    padded = (counts + ROW_BLOCK - 1) // ROW_BLOCK * ROW_BLOCK
    sorted_start = jnp.cumsum(counts) - counts
    padded_end = jnp.cumsum(padded)
    padded_start = padded_end - padded
    dest_sorted = padded_start[sorted_expert] + jnp.arange(ROUTE_ROWS) - sorted_start[sorted_expert]
    slot_token = jnp.full((NUM_BLOCKS * ROW_BLOCK,), NUM_TOKENS, jnp.int32).at[dest_sorted].set(row_order // TOP_K)
    dest_of_row = jnp.zeros((ROUTE_ROWS,), jnp.int32).at[row_order].set(dest_sorted)
    block_first = jnp.arange(NUM_BLOCKS) * ROW_BLOCK
    block_expert = jnp.minimum(jnp.sum(block_first[:, None] >= padded_end[None, :], axis=1), EXPERTS - 1)
    normed_pad = jnp.concatenate([normed, jnp.zeros((1, HIDDEN), normed.dtype)], axis=0)
    block_rows = normed_pad[slot_token].reshape(NUM_BLOCKS, ROW_BLOCK, HIDDEN)

    def one_block(block_in):
        block_x, expert_id = block_in
        expert_out = swiglu_rows(block_x, w_gate[expert_id], w_up[expert_id], w_down[expert_id])
        return expert_out.astype(jnp.bfloat16)

    padded_out = lax.map(one_block, (block_rows, block_expert)).reshape(NUM_BLOCKS * ROW_BLOCK, HIDDEN)
    row_out = padded_out[dest_of_row].reshape(NUM_TOKENS, TOP_K, HIDDEN)
    routed = jnp.sum(row_out.astype(jnp.float32) * route_w[:, :, None], axis=1)
    return (hidden.astype(jnp.float32) + shared_out + routed).astype(jnp.bfloat16)
```

```python
import functools

import jax
import jax.numpy as jnp
from jax import lax
from jax.experimental import pallas as pl
from jax.experimental.pallas import tpu as pltpu
from jax.sharding import PartitionSpec as P

NORM_EPS = 1e-6
QUAD = 4


def rms_norm(hidden, norm_gain):
    hidden_f32 = hidden.astype(jnp.float32)
    inv_rms = lax.rsqrt(jnp.mean(hidden_f32 * hidden_f32, axis=-1, keepdims=True) + NORM_EPS)
    return (hidden_f32 * inv_rms * norm_gain).astype(jnp.bfloat16)


def shared_swiglu(normed, shared_gate, shared_up, shared_down):
    gate_out = jnp.dot(normed, shared_gate, preferred_element_type=jnp.float32)
    up_out = jnp.dot(normed, shared_up, preferred_element_type=jnp.float32)
    activated = (jax.nn.silu(gate_out) * up_out).astype(jnp.bfloat16)
    return jnp.dot(activated, shared_down, preferred_element_type=jnp.float32)


def dense_weights(normed, router_w, topk_idx):
    logits = jnp.dot(normed, router_w, preferred_element_type=jnp.float32)
    probs = jax.nn.softmax(logits, axis=-1)
    experts = lax.broadcasted_iota(jnp.int32, (1, router_w.shape[1], 1), 1)
    chosen = jnp.any(topk_idx[:, None, :] == experts, axis=2)
    return jnp.where(chosen, probs, -1.0).T


def dispatch_kernel(slot_ref, rows_ref, out_ref, pick_ref):
    local_count, block_rows, hidden_size = out_ref.shape
    tokens = rows_ref.shape[0]
    row_id = lax.broadcasted_iota(jnp.int32, (block_rows, tokens), 0)
    for e in range(local_count):
        hit = row_id == slot_ref[0, e:e + 1, :]
        pick_ref[e * block_rows:(e + 1) * block_rows, :] = hit.astype(jnp.float32).astype(jnp.bfloat16)
    step = 512
    for n in range(0, hidden_size, step):
        got = jnp.dot(pick_ref[...], rows_ref[:, n:n + step], preferred_element_type=jnp.float32)
        got = got.astype(jnp.bfloat16)
        for e in range(local_count):
            out_ref[e, :, n:n + step] = got[e * block_rows:(e + 1) * block_rows]


def expert_kernel(x_ref, gate_ref, up_ref, down_ref, out_ref):
    x = x_ref[0]
    gate_out = jnp.dot(x, gate_ref[0], preferred_element_type=jnp.float32)
    up_out = jnp.dot(x, up_ref[0], preferred_element_type=jnp.float32)
    act = (jax.nn.silu(gate_out) * up_out).astype(jnp.bfloat16)
    out_ref[0] = jnp.dot(act, down_ref[0], preferred_element_type=jnp.float32).astype(jnp.bfloat16)


def combine_kernel(capacity, window, rank_ref, weight_ref, rows_ref, out_ref):
    local_count = rank_ref.shape[1]
    tokens, hidden_size = out_ref.shape[1:]
    place = lax.rem(pl.program_id(0), QUAD)
    shift = place * (capacity % 16)
    start = pl.multiple_of(place * (capacity - capacity % 16), 16)
    row_id = lax.broadcasted_iota(jnp.int32, (window, tokens), 0)
    parts = []
    rows = []
    for e in range(local_count):
        slot = rank_ref[0, e:e + 1, :]
        hit = (row_id == slot + shift) & (slot >= 0)
        parts.append(jnp.where(hit, weight_ref[0, e:e + 1, :], 0.0))
        rows.append(rows_ref[e, pl.ds(start, window), :])
    weight = jnp.concatenate(parts, axis=0)
    high = weight.astype(jnp.bfloat16)
    rest = weight - high.astype(jnp.float32)
    mid = rest.astype(jnp.bfloat16)
    low = (rest - mid.astype(jnp.float32)).astype(jnp.bfloat16)
    terms = jnp.concatenate([high, mid, low], axis=0).T
    rows = jnp.concatenate(rows * 3, axis=0)
    step = 512
    for n in range(0, hidden_size, step):
        out_ref[0, :, n:n + step] = jnp.dot(terms, rows[:, n:n + step], preferred_element_type=jnp.float32)


def solution(mesh):
    group_size = mesh.shape['ep']

    def local_step(hidden, norm_gain, router_w, topk_idx, w_gate, w_up, w_down, shared_gate, shared_up, shared_down):
        tok_count, hidden_size = hidden.shape
        top_k = topk_idx.shape[1]
        num_experts = router_w.shape[1]
        local_count, _, ff = w_gate.shape
        capacity = 3 * tok_count * top_k // (2 * num_experts)
        window = 48
        quads = group_size // QUAD
        block_rows = QUAD * capacity
        normed = rms_norm(hidden, norm_gain)
        weight_t = dense_weights(normed, router_w, topk_idx)
        all_weight = lax.all_gather(weight_t, 'ep', axis=0).reshape(group_size, group_size, local_count, tok_count)
        all_rows = lax.all_gather(normed, 'ep', axis=0, tiled=True)
        weight = lax.dynamic_index_in_dim(all_weight, lax.axis_index('ep'), 1, keepdims=False)
        chosen = weight >= 0
        before = jnp.triu(jnp.ones((tok_count, tok_count), jnp.bfloat16), 1)
        rank = jnp.einsum('set,tu->seu', chosen.astype(jnp.bfloat16), before, preferred_element_type=jnp.float32)
        rank = jnp.where(chosen, rank.astype(jnp.int32), -1)
        offset = (jnp.arange(group_size, dtype=jnp.int32) % QUAD * capacity)[:, None, None]
        slot = jnp.where(chosen, rank + offset, -1).reshape(quads, QUAD, local_count, tok_count)
        slot = slot.swapaxes(1, 2).reshape(quads, local_count, QUAD * tok_count)
        params = pltpu.CompilerParams(vmem_limit_bytes=60 * 1024 * 1024)
        expert_in = pl.pallas_call(
            dispatch_kernel,
            grid=(quads,),
            in_specs=[pl.BlockSpec((1, local_count, QUAD * tok_count), lambda q: (q, 0, 0)),
                      pl.BlockSpec((QUAD * tok_count, hidden_size), lambda q: (q, 0))],
            out_specs=pl.BlockSpec((local_count, block_rows, hidden_size), lambda q: (0, q, 0)),
            out_shape=jax.ShapeDtypeStruct((local_count, quads * block_rows, hidden_size), jnp.bfloat16),
            scratch_shapes=[pltpu.VMEM((local_count * block_rows, QUAD * tok_count), jnp.bfloat16)],
            compiler_params=params,
            name='dispatch',
        )(slot, all_rows)
        total_rows = quads * block_rows
        expert_out = pl.pallas_call(
            expert_kernel,
            grid=(local_count,),
            in_specs=[pl.BlockSpec((1, total_rows, hidden_size), lambda e: (e, 0, 0)),
                      pl.BlockSpec((1, hidden_size, ff), lambda e: (e, 0, 0)),
                      pl.BlockSpec((1, hidden_size, ff), lambda e: (e, 0, 0)),
                      pl.BlockSpec((1, ff, hidden_size), lambda e: (e, 0, 0))],
            out_specs=pl.BlockSpec((1, total_rows, hidden_size), lambda e: (e, 0, 0)),
            out_shape=jax.ShapeDtypeStruct((local_count, total_rows, hidden_size), jnp.bfloat16),
            compiler_params=params,
            name='experts',
        )(expert_in, w_gate, w_up, w_down)
        partial = pl.pallas_call(
            functools.partial(combine_kernel, capacity, window),
            grid=(group_size,),
            in_specs=[pl.BlockSpec((1, local_count, tok_count), lambda s: (s, 0, 0)),
                      pl.BlockSpec((1, local_count, tok_count), lambda s: (s, 0, 0)),
                      pl.BlockSpec((local_count, block_rows, hidden_size), lambda s: (0, s // QUAD, 0))],
            out_specs=pl.BlockSpec((1, tok_count, hidden_size), lambda s: (s, 0, 0)),
            out_shape=jax.ShapeDtypeStruct((group_size, tok_count, hidden_size), jnp.float32),
            compiler_params=params,
            name='combine',
        )(rank, weight, expert_out)
        routed = lax.psum_scatter(partial, 'ep', scatter_dimension=0, tiled=False)
        shared_out = shared_swiglu(normed, shared_gate, shared_up, shared_down)
        return (hidden.astype(jnp.float32) + shared_out + routed).astype(jnp.bfloat16)

    token_spec = P(('dp', 'ep'), None)
    expert_spec = P('ep', None, None)
    return jax.shard_map(
        local_step,
        mesh=mesh,
        in_specs=(token_spec, P(None), P(None, None), token_spec, expert_spec, expert_spec, expert_spec,
                  P(None, None), P(None, None), P(None, None)),
        out_specs=token_spec,
        check_vma=False,
    )
```

```python
import functools

import jax
import jax.numpy as jnp
from jax import lax
from jax.experimental import pallas as pl
from jax.experimental.pallas import tpu as pltpu
from jax.sharding import PartitionSpec as P

NORM_EPS = 1e-6
CORES = 2
VMEM_LIMIT = 67043328
F32 = jnp.float32
BF16 = jnp.bfloat16


def rms_norm(hidden, norm_gain):
    hidden_f32 = hidden.astype(F32)
    inv_rms = lax.rsqrt(jnp.mean(hidden_f32 * hidden_f32, axis=-1, keepdims=True) + NORM_EPS)
    return (hidden_f32 * inv_rms * norm_gain).astype(BF16)


def side_rows(normed, router_w, topk_idx):
    logits = jnp.dot(normed, router_w, preferred_element_type=F32)
    probs = jax.nn.softmax(logits, axis=-1).T
    idx = topk_idx.T
    top_k, tokens = idx.shape
    experts = lax.broadcasted_iota(jnp.int32, (1, probs.shape[0], 1), 1)
    weight = jnp.sum(jnp.where(idx[:, None, :] == experts, probs[None], 0.0), axis=1)
    fill = jnp.full((8 - top_k, tokens), -1.0, F32)
    return jnp.concatenate([idx.astype(F32), fill, weight, fill], axis=0)


def slots_of(side, first_expert, local_count, before):
    ids, weights = side[0:8], side[8:16]
    chosen, picked = [], []
    for e in range(8):
        hit = ids == (first_expert + e).astype(F32)
        chosen.append(jnp.sum(jnp.where(hit, 1.0, 0.0), axis=0, keepdims=True))
        picked.append(jnp.sum(jnp.where(hit, weights, 0.0), axis=0, keepdims=True))
    chosen = jnp.concatenate(chosen, axis=0)
    rank = jnp.dot(chosen.astype(BF16), before, preferred_element_type=F32)
    slot = jnp.where(chosen > 0.5, rank, -1000.0)
    return [slot[e:e + 1] for e in range(local_count)], picked[:local_count]


def place_of(group_size):
    chips = group_size // CORES
    me = lax.axis_index('ep')
    chip, core = me // CORES, me % CORES
    right = (chip + 1) % chips * CORES + core
    left = (chip + chips - 1) % chips * CORES + core
    return me, chip, core, right, left, chip * CORES + (1 - core)


def enter(neighbours):
    barrier = pltpu.get_barrier_semaphore()
    for device in neighbours:
        pl.semaphore_signal(barrier, inc=1, device_id={'ep': device}, device_id_type=pl.DeviceIdType.MESH)
    pl.semaphore_wait(barrier, len(neighbours))


def remote(src, dst, send_sem, recv_sem, device):
    return pltpu.make_async_remote_copy(src_ref=src, dst_ref=dst, send_sem=send_sem, recv_sem=recv_sem,
                                        device_id={'ep': device}, device_id_type=pl.DeviceIdType.MESH)


def gather_kernel(group_size, capacity, slots, rows_hbm, side_hbm, before_ref, sgate, sup, sdown, wgate, wup, wdown,
                  out_hbm, side_out, shared_ref,
                  rows, sides, x_ref, pick, gate_buf, up_buf, down_buf, stage,
                  ring_s, ring_r, part_s, part_r, tring_s, tring_r, tpart_s, tpart_r, own_s, own_r, load_sem, w_sem, out_sem):
    me, _, core, right, left, partner = place_of(group_size)
    local_count, hidden_size, ff = wgate.shape
    tokens = rows_hbm.shape[0]
    half = tokens // 2
    last = group_size // CORES - 1
    mine = pl.multiple_of(core * tokens, tokens)
    other = pl.multiple_of((1 - core) * tokens, tokens)

    def order(way, n):
        return min(2 * n + 1 + way, last)

    def piece(way, i, base):
        r = i % 2 if way == 0 else 1 - i % 2
        return rows.at[order(way, i // 2), pl.ds(pl.multiple_of(base + r * half, half), half)]

    def ring(way, i):
        n = i // 2
        r = i % 2 if way == 0 else 1 - i % 2
        src = 0 if n == 0 else order(way, n - 1)
        return remote(rows.at[src, pl.ds(pl.multiple_of(mine + r * half, half), half)], piece(way, i, mine),
                      ring_s.at[way, i], ring_r.at[way, i], right if way == 0 else left)

    def part(way, i, base):
        return remote(piece(way, i, base), piece(way, i, base), part_s.at[way, i], part_r.at[way, i], partner)

    def tring(way, n):
        src = 0 if n == 0 else 2 * (n - 1) + 1 + way
        return remote(sides.at[src, core], sides.at[2 * n + 1 + way, core],
                      tring_s.at[way, n], tring_r.at[way, n], right if way == 0 else left)

    def tpart(way, n, who):
        place = sides.at[2 * n + 1 + way, who]
        return remote(place, place, tpart_s.at[way, n], tpart_r.at[way, n], partner)

    def own_part(base):
        place = rows.at[0, pl.ds(base, tokens)]
        return remote(place, place, own_s.at[0], own_r.at[0], partner)

    def own_tpart(who):
        place = sides.at[0, who]
        return remote(place, place, own_s.at[1], own_r.at[1], partner)

    sends = 7

    def send(i):
        for way in range(2):
            ring(way, i).start()
            if i % 2 == 0:
                tring(way, i // 2).start()

    def service(i):
        for way in range(2):
            ring(way, i).wait_recv()
            if i % 2 == 0:
                tring(way, i // 2).wait_recv()
        if i + 2 < sends:
            send(i + 2)
        for way in range(2):
            part(way, i, mine).start()
            if i % 2 == 0:
                tpart(way, i // 2, core).start()

    def partner_arrived(i):
        for way in range(2):
            part(way, i, other).wait_recv()
            if i % 2 == 0:
                tpart(way, i // 2, 1 - core).wait_recv()

    load_rows = pltpu.make_async_copy(rows_hbm, rows.at[0, pl.ds(mine, tokens)], load_sem.at[0])
    load_side = pltpu.make_async_copy(side_hbm, sides.at[0, core], load_sem.at[1])
    load_rows.start()
    load_side.start()

    def gate_copies(slot, gate, up):
        return (pltpu.make_async_copy(gate, gate_buf.at[slot], w_sem.at[slot]),
                pltpu.make_async_copy(up, up_buf.at[slot], w_sem.at[2 + slot]))

    def start_gate(slot, gate, up):
        for copy in gate_copies(slot, gate, up):
            copy.start()

    def down_copy(down):
        return pltpu.make_async_copy(down, down_buf, w_sem.at[4])

    def shared_cols(ref, i):
        return ref.at[:, i * ff:(i + 1) * ff]

    start_gate(0, shared_cols(sgate, 0), shared_cols(sup, 0))
    enter((right, left, partner))
    load_rows.wait()
    load_side.wait()
    send(0)
    send(1)
    own_part(mine).start()
    own_tpart(core).start()

    def activate(x, slot):
        for copy in gate_copies(slot, wgate.at[0], wup.at[0]):
            copy.wait()
        gate_out = jnp.dot(x, gate_buf[slot], preferred_element_type=F32)
        up_out = jnp.dot(x, up_buf[slot], preferred_element_type=F32)
        return (jax.nn.silu(gate_out) * up_out).astype(BF16)

    def project(act):
        down_copy(wdown.at[0]).wait()
        return jnp.dot(act, down_buf[...], preferred_element_type=F32)

    x_own = rows[0, pl.ds(mine, tokens), :]
    down_copy(sdown.at[0:ff]).start()
    start_gate(1, shared_cols(sgate, 1), shared_cols(sup, 1))
    shared_ref[...] = project(activate(x_own, 0))
    down_copy(sdown.at[ff:2 * ff]).start()
    start_gate(0, wgate.at[0], wup.at[0])
    x_own = rows[0, pl.ds(mine, tokens), :]
    shared_ref[...] += project(activate(x_own, 1))

    def dispatch(base, start, count):
        def one(ch, carry):
            for cc in range(CORES):
                slot, _ = slots_of(sides[ch, cc], me * local_count, local_count, before_ref[...])
                row_id = lax.broadcasted_iota(jnp.int32, (slots, tokens), 0).astype(F32)
                for e in range(local_count):
                    hit = row_id == slot[e] + float(capacity * cc)
                    pick[e * slots:(e + 1) * slots, cc * tokens:(cc + 1) * tokens] = jnp.where(hit, 1.0, 0.0).astype(BF16)
            step = min(512, hidden_size)
            for n in range(0, hidden_size, step):
                got = jnp.dot(pick[...], rows[ch, :, n:n + step], preferred_element_type=F32).astype(BF16)
                for e in range(local_count):
                    x_ref[e, ch - base, :, n:n + step] = got[e * slots:(e + 1) * slots]
            return carry
        lax.fori_loop(start, start + count, one, 0)

    def stage_copy(e, first, count):
        return pltpu.make_async_copy(stage.at[0:count], out_hbm.at[e, pl.ds(first, count)], out_sem.at[0])

    def experts(first, count, begin, end, final):
        def one(e, carry):
            slot = e % 2
            down_copy(wdown.at[e]).start()
            following = (e + 1) % local_count
            if final:
                @pl.when(e < local_count - 1)
                def _():
                    start_gate(1 - slot, wgate.at[following], wup.at[following])
            else:
                start_gate(1 - slot, wgate.at[following], wup.at[following])
            x = x_ref[e, 0:count].reshape(count * slots, hidden_size)
            out = project(activate(x, slot)).astype(BF16)

            @pl.when(e > 0)
            def _():
                stage_copy(e - 1, first, count).wait()
            stage[0:count] = out.reshape(count, slots, hidden_size)
            stage_copy(e, first, count).start()
            return carry
        lax.fori_loop(begin, end, one, 0)

    def finish(first, count):
        stage_copy(local_count - 1, first, count).wait()

    service(0)
    own_part(other).wait_recv()
    own_tpart(1 - core).wait_recv()
    dispatch(0, 0, 1)
    service(1)
    partner_arrived(0)
    partner_arrived(1)
    dispatch(0, 1, 2)
    experts(0, 3, 0, 2, False)
    service(2)
    experts(0, 3, 2, 4, False)
    finish(0, 3)
    service(3)
    partner_arrived(2)
    partner_arrived(3)
    dispatch(3, 3, 2)
    experts(3, 2, 0, 2, False)
    service(4)
    experts(3, 2, 2, 4, False)
    finish(3, 2)
    service(5)
    partner_arrived(4)
    partner_arrived(5)
    dispatch(5, 5, 2)
    service(6)
    partner_arrived(6)
    dispatch(5, 7, 1)
    experts(5, 3, 0, 4, True)
    finish(5, 3)
    side_out[...] = sides[0:group_size // CORES]
    for way in range(2):
        for i in range(sends):
            ring(way, i).wait_send()
            part(way, i, mine).wait_send()
            if i % 2 == 0:
                tring(way, i // 2).wait_send()
                tpart(way, i // 2, core).wait_send()
    own_part(mine).wait_send()
    own_tpart(core).wait_send()


def scatter_kernel(group_size, capacity, slots, rows_hbm, side_ref, before_ref, hidden_ref, shared_ref, out_ref,
                   rows, acc, part_in, ring_in, load_sem, ring_s, ring_r, part_s, part_r):
    me, _, core, right, left, partner = place_of(group_size)
    local_count, chips, _, hidden_size = rows.shape
    tokens = hidden_ref.shape[0]
    half = hidden_size // 2
    last = chips - 1
    sends = 7

    def load(ch):
        return pltpu.make_async_copy(rows_hbm.at[:, ch], rows.at[:, ch], load_sem.at[ch])

    need = [last, last - 1, last - 2, 4, 3, 2, 1, 0]
    for ch in need:
        load(ch).start()

    def ring(way, i):
        return remote(acc.at[0, way, i % 2], ring_in.at[way, i], ring_s.at[way, i], ring_r.at[way, i],
                      right if way == 0 else left)

    def part(way, i):
        return remote(acc.at[1, way, i % 2], part_in.at[way, i], part_s.at[way, i], part_r.at[way, i], partner)

    def unit(ch, cc, h):
        slot, weight = slots_of(side_ref[ch, cc], me * local_count, local_count, before_ref[...])
        row_id = lax.broadcasted_iota(jnp.int32, (WINDOW, tokens), 0).astype(F32)
        shift = (cc * (capacity - 32)).astype(F32)
        mix = jnp.concatenate([jnp.where(row_id == slot[e] + shift, weight[e], 0.0) for e in range(local_count)], axis=0)
        high = mix.astype(BF16)
        rest = mix - high.astype(F32)
        mid = rest.astype(BF16)
        low = (rest - mid.astype(F32)).astype(BF16)
        start = pl.multiple_of(cc * 32, 32)
        col = pl.multiple_of(h * half, half)
        picked = jnp.concatenate([rows[e, ch, pl.ds(start, WINDOW), pl.ds(col, half)] for e in range(local_count)], axis=0)
        total = jnp.dot(high.T, picked, preferred_element_type=F32)
        total += jnp.dot(mid.T, picked, preferred_element_type=F32)
        return total + jnp.dot(low.T, picked, preferred_element_type=F32)

    def units(i, chans, halves):
        def one(step, carry):
            who, way = 1 - step // 2, step % 2
            ch = chans[0] + way * (chans[1] - chans[0])
            h = halves[0] + way * (halves[1] - halves[0])
            cc = core + who - 2 * core * who
            acc[who, way, i % 2] = unit(ch, cc, h)
            return carry
        lax.fori_loop(0, 4, one, 0)

    enter((right, left, partner))
    loaded = set()

    def ensure(ch):
        if ch not in loaded:
            loaded.add(ch)
            load(ch).wait()

    for i in range(sends):
        k = 4 - (i + 1) // 2
        chans = (min(2 * k, last), 2 * k - 1)
        for ch in chans:
            ensure(ch)
        if i >= 2:
            for way in range(2):
                ring(way, i - 2).wait_send()
                part(way, i - 2).wait_send()
        units(i, chans, (i % 2, 1 - i % 2))
        for way in range(2):
            part(way, i).start()
        for way in range(2):
            part(way, i).wait_recv()
            if i >= 2:
                ring(way, i - 2).wait_recv()
                acc[0, way, i % 2] = acc[0, way, i % 2] + part_in[way, i] + ring_in[way, i - 2]
            else:
                acc[0, way, i % 2] = acc[0, way, i % 2] + part_in[way, i]
            ring(way, i).start()
    ensure(0)
    for way in range(2):
        ring(way, sends - 2).wait_send()
        part(way, sends - 2).wait_send()
    units(sends, (0, 0), (0, 1))
    for way in range(2):
        part(way, sends).start()
    for h in range(2):
        part(h, sends).wait_recv()
        ring(1 - h, sends - 2).wait_recv()
        cols = slice(h * half, (h + 1) * half)
        acc[0, h, sends % 2] = (acc[0, h, sends % 2] + part_in[h, sends] + ring_in[1 - h, sends - 2]
                                + shared_ref[:, cols] + hidden_ref[:, cols].astype(F32))
    for h in range(2):
        ring(h, sends - 1).wait_recv()
        cols = slice(h * half, (h + 1) * half)
        out_ref[:, cols] = (acc[0, h, sends % 2] + ring_in[h, sends - 1]).astype(BF16)
    for way in range(2):
        ring(way, sends - 1).wait_send()
        part(way, sends - 1).wait_send()
        part(way, sends).wait_send()


WINDOW = 48


def solution(mesh):
    group_size = mesh.shape['ep']
    chips = group_size // CORES

    def local_step(hidden, norm_gain, router_w, topk_idx, w_gate, w_up, w_down, shared_gate, shared_up, shared_down):
        tokens, hidden_size = hidden.shape
        num_experts = router_w.shape[1]
        local_count, _, ff = w_gate.shape
        capacity = 3 * tokens * topk_idx.shape[1] // (2 * num_experts)
        slots = (CORES * capacity + 15) // 16 * 16
        normed = rms_norm(hidden, norm_gain)
        side = side_rows(normed, router_w, topk_idx)
        before = jnp.triu(jnp.ones((tokens, tokens), BF16), 1)
        hbm = pl.BlockSpec(memory_space=pl.ANY)
        vmem = pl.BlockSpec(memory_space=pltpu.VMEM)
        dma = pltpu.SemaphoreType.DMA
        expert_out, sides, shared_out = pl.pallas_call(
            functools.partial(gather_kernel, group_size, capacity, slots),
            in_specs=[hbm, hbm, vmem] + [hbm] * 6,
            out_specs=(hbm, vmem, vmem),
            out_shape=(jax.ShapeDtypeStruct((local_count, chips, slots, hidden_size), BF16),
                       jax.ShapeDtypeStruct((chips, CORES, 16, tokens), F32),
                       jax.ShapeDtypeStruct((tokens, hidden_size), F32)),
            scratch_shapes=[
                pltpu.VMEM((chips, CORES * tokens, hidden_size), BF16),
                pltpu.VMEM((chips + 1, CORES, 16, tokens), F32),
                pltpu.VMEM((local_count, 3, slots, hidden_size), BF16),
                pltpu.VMEM((local_count * slots, CORES * tokens), BF16),
                pltpu.VMEM((2, hidden_size, ff), BF16),
                pltpu.VMEM((2, hidden_size, ff), BF16),
                pltpu.VMEM((ff, hidden_size), BF16),
                pltpu.VMEM((3, slots, hidden_size), BF16),
                dma((2, 7)), dma((2, 7)), dma((2, 7)), dma((2, 7)),
                dma((2, 4)), dma((2, 4)), dma((2, 4)), dma((2, 4)),
                dma((2,)), dma((2,)), dma((2,)), dma((5,)), dma((1,)),
            ],
            compiler_params=pltpu.CompilerParams(collective_id=0, has_side_effects=True, vmem_limit_bytes=VMEM_LIMIT),
            name='gather_experts',
        )(normed, side, before, shared_gate, shared_up, shared_down, w_gate, w_up, w_down)
        return pl.pallas_call(
            functools.partial(scatter_kernel, group_size, capacity, slots),
            in_specs=[hbm, vmem, vmem, vmem, vmem],
            out_specs=vmem,
            out_shape=jax.ShapeDtypeStruct((tokens, hidden_size), BF16),
            scratch_shapes=[
                pltpu.VMEM((local_count, chips, slots, hidden_size), BF16),
                pltpu.VMEM((2, 2, 2, tokens, hidden_size // 2), F32),
                pltpu.VMEM((2, 8, tokens, hidden_size // 2), F32),
                pltpu.VMEM((2, 7, tokens, hidden_size // 2), F32),
                dma((chips,)), dma((2, 7)), dma((2, 7)), dma((2, 8)), dma((2, 8)),
            ],
            compiler_params=pltpu.CompilerParams(collective_id=1, has_side_effects=True, vmem_limit_bytes=VMEM_LIMIT),
            name='combine_scatter',
        )(expert_out, sides, before, hidden, shared_out)

    token_spec = P(('dp', 'ep'), None)
    expert_spec = P('ep', None, None)
    return jax.shard_map(
        local_step,
        mesh=mesh,
        in_specs=(token_spec, P(None), P(None, None), token_spec, expert_spec, expert_spec, expert_spec,
                  P(None, None), P(None, None), P(None, None)),
        out_specs=token_spec,
        check_vma=False,
    )
```

```python
import functools

import jax
import jax.numpy as jnp
from jax import lax
from jax.experimental import pallas as pl
from jax.experimental.pallas import tpu as pltpu
from jax.sharding import PartitionSpec as P

NORM_EPS = 1e-6
CORES = 2
VMEM_LIMIT = 67043328
F32 = jnp.float32
BF16 = jnp.bfloat16


def slots_of(side, first_expert, local_count, before):
    ids, weights = side[0:8], side[8:16]
    chosen, picked = [], []
    for e in range(8):
        hit = ids == (first_expert + e).astype(F32)
        chosen.append(jnp.sum(jnp.where(hit, 1.0, 0.0), axis=0, keepdims=True))
        picked.append(jnp.sum(jnp.where(hit, weights, 0.0), axis=0, keepdims=True))
    chosen = jnp.concatenate(chosen, axis=0)
    rank = jnp.dot(chosen.astype(BF16), before, preferred_element_type=F32)
    slot = jnp.where(chosen > 0.5, rank, -1000.0)
    return [slot[e:e + 1] for e in range(local_count)], picked[:local_count]


def place_of(group_size):
    chips = group_size // CORES
    me = lax.axis_index('ep')
    chip, core = me // CORES, me % CORES
    right = (chip + 1) % chips * CORES + core
    left = (chip + chips - 1) % chips * CORES + core
    return me, chip, core, right, left, chip * CORES + (1 - core)


def enter(neighbours):
    barrier = pltpu.get_barrier_semaphore()
    for device in neighbours:
        pl.semaphore_signal(barrier, inc=1, device_id={'ep': device}, device_id_type=pl.DeviceIdType.MESH)
    pl.semaphore_wait(barrier, len(neighbours))


def remote(src, dst, send_sem, recv_sem, device):
    return pltpu.make_async_remote_copy(src_ref=src, dst_ref=dst, send_sem=send_sem, recv_sem=recv_sem,
                                        device_id={'ep': device}, device_id_type=pl.DeviceIdType.MESH)


def gather_kernel(group_size, capacity, slots, hidden_hbm, gain_ref, router_ref, idx_ref, before_ref,
                  sgate, sup, sdown, wgate, wup, wdown,
                  out_hbm, head_hbm, side_out, shared_ref,
                  rows, sides, x_ref, pick, gate_buf, up_buf, down_buf,
                  ring_s, ring_r, part_s, part_r, tring_s, tring_r, tpart_s, tpart_r, own_s, own_r,
                  head_s, head_r, load_sem, w_sem, out_sem):
    me, _, core, right, left, partner = place_of(group_size)
    local_count, hidden_size, ff = wgate.shape
    tokens = hidden_hbm.shape[0]
    half = tokens // 2
    half_cols = hidden_size // 2
    last = group_size // CORES - 1
    mine = pl.multiple_of(core * tokens, tokens)
    other = pl.multiple_of((1 - core) * tokens, tokens)

    def order(way, n):
        return min(2 * n + 1 + way, last)

    def piece(way, i, base):
        r = i % 2 if way == 0 else 1 - i % 2
        return rows.at[order(way, i // 2), pl.ds(pl.multiple_of(base + r * half, half), half)]

    def ring(way, i):
        n = i // 2
        r = i % 2 if way == 0 else 1 - i % 2
        src = 0 if n == 0 else order(way, n - 1)
        return remote(rows.at[src, pl.ds(pl.multiple_of(mine + r * half, half), half)], piece(way, i, mine),
                      ring_s.at[way, i], ring_r.at[way, i], right if way == 0 else left)

    def part(way, i, base):
        return remote(piece(way, i, base), piece(way, i, base), part_s.at[way, i], part_r.at[way, i], partner)

    def tring(way, n):
        src = 0 if n == 0 else 2 * (n - 1) + 1 + way
        return remote(sides.at[src, core], sides.at[2 * n + 1 + way, core],
                      tring_s.at[way, n], tring_r.at[way, n], right if way == 0 else left)

    def tpart(way, n, who):
        place = sides.at[2 * n + 1 + way, who]
        return remote(place, place, tpart_s.at[way, n], tpart_r.at[way, n], partner)

    def own_part(base):
        place = rows.at[0, pl.ds(base, tokens)]
        return remote(place, place, own_s.at[0], own_r.at[0], partner)

    def own_tpart(who):
        place = sides.at[0, who]
        return remote(place, place, own_s.at[1], own_r.at[1], partner)

    sends = 7

    def send(i):
        for way in range(2):
            ring(way, i).start()
            if i % 2 == 0 and i > 0:
                tring(way, i // 2).start()

    def service(i):
        for way in range(2):
            ring(way, i).wait_recv()
            if i % 2 == 0:
                tring(way, i // 2).wait_recv()
        if i + 2 < sends:
            send(i + 2)
        for way in range(2):
            part(way, i, mine).start()
            if i % 2 == 0:
                tpart(way, i // 2, core).start()

    def partner_arrived(i):
        for way in range(2):
            part(way, i, other).wait_recv()
            if i % 2 == 0:
                tpart(way, i // 2, 1 - core).wait_recv()

    def head(way, step, e):
        chip_row, cols = (((2, 0), (1, 1)), ((2, 1), (0, 0)))[way][step]
        return remote(x_ref.at[e, chip_row, :, cols * half_cols:(cols + 1) * half_cols], head_hbm.at[way, step, e],
                      head_s.at[way, step, e], head_r.at[way, step, e], right if way == 0 else left)

    load_rows = pltpu.make_async_copy(hidden_hbm, rows.at[0, pl.ds(mine, tokens)], load_sem.at[0])
    load_rows.start()

    def normalise():
        block = 32

        def one(i, carry):
            place = pl.ds(pl.multiple_of(mine + i * block, block), block)
            x = rows[0, place, :].astype(F32)
            inv_rms = lax.rsqrt(jnp.mean(x * x, axis=-1, keepdims=True) + NORM_EPS)
            rows[0, place, :] = (x * inv_rms * gain_ref[...]).astype(BF16)
            return carry
        lax.fori_loop(0, tokens // block, one, 0)

    def route():
        x = rows[0, pl.ds(mine, tokens), :]
        logits = lax.dot_general(router_ref[...], x, (((1,), (1,)), ((), ())), preferred_element_type=F32)
        top = jnp.exp(logits - jnp.max(logits, axis=0, keepdims=True))
        probs = top / jnp.sum(top, axis=0, keepdims=True)
        experts_id = lax.broadcasted_iota(jnp.int32, probs.shape, 0)
        sides[0, core] = jnp.full((16, tokens), -1.0, F32)
        for j in range(idx_ref.shape[0]):
            idx = idx_ref[j:j + 1, :]
            sides[0, core, j:j + 1, :] = idx.astype(F32)
            sides[0, core, 8 + j:9 + j, :] = jnp.sum(jnp.where(experts_id == idx, probs, 0.0), axis=0, keepdims=True)

    def gate_copies(slot, gate, up):
        return (pltpu.make_async_copy(gate, gate_buf.at[slot], w_sem.at[slot]),
                pltpu.make_async_copy(up, up_buf.at[slot], w_sem.at[2 + slot]))

    def start_gate(slot, gate, up):
        for copy in gate_copies(slot, gate, up):
            copy.start()

    def down_copy(down):
        return pltpu.make_async_copy(down, down_buf, w_sem.at[4])

    def shared_cols(ref, i):
        return ref.at[:, pl.ds(pl.multiple_of(i * ff, 128), ff)]

    start_gate(0, shared_cols(sgate, 0), shared_cols(sup, 0))
    enter((right, left, partner))
    load_rows.wait()
    normalise()
    send(0)
    send(1)
    own_part(mine).start()
    route()
    for way in range(2):
        tring(way, 0).start()
    own_tpart(core).start()

    def activate(x, slot):
        for copy in gate_copies(slot, wgate.at[0], wup.at[0]):
            copy.wait()
        gate_out = jnp.dot(x, gate_buf[slot], preferred_element_type=F32)
        up_out = jnp.dot(x, up_buf[slot], preferred_element_type=F32)
        return (jax.nn.silu(gate_out) * up_out).astype(BF16)

    def project(act):
        down_copy(wdown.at[0]).wait()
        return jnp.dot(act, down_buf[...], preferred_element_type=F32)

    shared_parts = sgate.shape[1] // ff

    def shared(i, carry):
        slot = i % 2
        down_copy(sdown.at[pl.ds(pl.multiple_of(i * ff, 128), ff)]).start()

        @pl.when(i < shared_parts - 1)
        def _():
            start_gate(1 - slot, shared_cols(sgate, i + 1), shared_cols(sup, i + 1))

        @pl.when(i == shared_parts - 1)
        def _():
            start_gate(1 - slot, wgate.at[0], wup.at[0])
        shared_ref[...] += project(activate(rows[0, pl.ds(mine, tokens), :], slot))
        return carry

    shared_ref[...] = jnp.zeros_like(shared_ref)
    lax.fori_loop(0, shared_parts, shared, 0)

    def dispatch(base, start, count):
        def one(ch, carry):
            for cc in range(CORES):
                slot, _ = slots_of(sides[ch, cc], me * local_count, local_count, before_ref[...])
                row_id = lax.broadcasted_iota(jnp.int32, (slots, tokens), 0).astype(F32)
                for e in range(local_count):
                    hit = row_id == slot[e] + float(capacity * cc)
                    pick[e * slots:(e + 1) * slots, cc * tokens:(cc + 1) * tokens] = jnp.where(hit, 1.0, 0.0).astype(BF16)
            step = min(512, hidden_size)
            for n in range(0, hidden_size, step):
                got = jnp.dot(pick[...], rows[ch, :, n:n + step], preferred_element_type=F32).astype(BF16)
                for e in range(local_count):
                    x_ref[e, ch - base, :, n:n + step] = got[e * slots:(e + 1) * slots]
            return carry
        lax.fori_loop(start, start + count, one, 0)

    def stage_copy(e, first, count):
        return pltpu.make_async_copy(x_ref.at[e, 0:count], out_hbm.at[e, pl.ds(first, count)], out_sem.at[e])

    def experts(first, count, middle):
        final = middle is None

        def one(e, carry):
            slot = e % 2
            if middle is not None:
                @pl.when(e == local_count // 2)
                def _():
                    service(middle)
            down_copy(wdown.at[e]).start()
            following = (e + 1) % local_count
            if final:
                @pl.when(e < local_count - 1)
                def _():
                    start_gate(1 - slot, wgate.at[following], wup.at[following])
            else:
                start_gate(1 - slot, wgate.at[following], wup.at[following])
            x = x_ref[e, 0:count].reshape(count * slots, hidden_size)
            out = project(activate(x, slot)).astype(BF16)
            x_ref[e, 0:count] = out.reshape(count, slots, hidden_size)
            if final:
                for step in range(2):
                    for way in range(2):
                        head(way, step, e).start()
            stage_copy(e, first, count).start()
            return carry
        lax.fori_loop(0, local_count, one, 0)

    def finish(first, count):
        for e in range(local_count):
            stage_copy(e, first, count).wait()

    service(0)
    own_part(other).wait_recv()
    own_tpart(1 - core).wait_recv()
    dispatch(0, 0, 1)
    service(1)
    partner_arrived(0)
    partner_arrived(1)
    dispatch(0, 1, 2)
    experts(0, 3, 2)
    finish(0, 3)
    service(3)
    partner_arrived(2)
    partner_arrived(3)
    dispatch(3, 3, 2)
    experts(3, 2, 4)
    finish(3, 2)
    service(5)
    partner_arrived(4)
    partner_arrived(5)
    dispatch(5, 5, 2)
    service(6)
    partner_arrived(6)
    dispatch(5, 7, 1)
    experts(5, 3, None)
    finish(5, 3)
    side_out[...] = sides[0:group_size // CORES]
    for way in range(2):
        for i in range(sends):
            ring(way, i).wait_send()
            part(way, i, mine).wait_send()
            if i % 2 == 0:
                tring(way, i // 2).wait_send()
                tpart(way, i // 2, core).wait_send()
    own_part(mine).wait_send()
    own_tpart(core).wait_send()
    for step in range(2):
        for way in range(2):
            for e in range(local_count):
                head(way, step, e).wait_recv()
                head(way, step, e).wait_send()


def scatter_kernel(group_size, capacity, rows_hbm, head_hbm, side_ref, before_ref, hidden_ref, shared_ref, out_ref,
                   rows, heads, acc, part_in, ring_in, load_sem, head_sem, ring_s, ring_r, part_s, part_r):
    me, _, core, right, left, partner = place_of(group_size)
    local_count, chips, _, hidden_size = rows.shape
    tokens = hidden_ref.shape[0]
    half = hidden_size // 2
    last = chips - 1
    steps = 5

    def load(ch):
        return pltpu.make_async_copy(rows_hbm.at[:, ch], rows.at[:, ch], load_sem.at[ch])

    def load_head(way, i):
        return pltpu.make_async_copy(head_hbm.at[way, i], heads.at[way, i], head_sem.at[way, i])

    for i in range(2):
        for way in range(2):
            load_head(way, i).start()
            load((last - 1, last - 2, 4, 3)[2 * i + way]).start()
    for ch in (2, 1, 0):
        load(ch).start()

    def ring(way, i):
        return remote(acc.at[0, way, i % 2], ring_in.at[way, i], ring_s.at[way, i], ring_r.at[way, i],
                      right if way == 0 else left)

    def part(way, i):
        return remote(acc.at[1, way, i % 2], part_in.at[way, i], part_s.at[way, i], part_r.at[way, i], partner)

    def mix_of(ch, cc, device):
        slot, weight = slots_of(side_ref[ch, cc], device * local_count, local_count, before_ref[...])
        row_id = lax.broadcasted_iota(jnp.int32, (WINDOW, tokens), 0).astype(F32)
        shift = (cc * (capacity - 32)).astype(F32)
        return [jnp.where(row_id == slot[e] + shift, weight[e], 0.0) for e in range(local_count)]

    def unit(ch, cc, h, way, i):
        start = pl.multiple_of(cc * 32, 32)
        col = pl.multiple_of(h * half, half)
        mix = mix_of(ch, cc, me)
        picked = [rows[e, ch, pl.ds(start, WINDOW), pl.ds(col, half)] for e in range(local_count)]
        if i < 2:
            mix += mix_of(ch, cc, left + way * (right - left))
            picked += [heads[way, i, e, pl.ds(start, WINDOW), :] for e in range(local_count)]
        mix = jnp.concatenate(mix, axis=0)
        picked = jnp.concatenate(picked, axis=0)
        high = mix.astype(BF16)
        rest = mix - high.astype(F32)
        mid = rest.astype(BF16)
        low = (rest - mid.astype(F32)).astype(BF16)
        total = jnp.dot(high.T, picked, preferred_element_type=F32)
        total += jnp.dot(mid.T, picked, preferred_element_type=F32)
        return total + jnp.dot(low.T, picked, preferred_element_type=F32)

    def units(i, chans, halves):
        def one(step, carry):
            who, way = 1 - step // 2, step % 2
            ch = chans[0] + way * (chans[1] - chans[0])
            h = halves[0] + way * (halves[1] - halves[0])
            cc = core + who - 2 * core * who
            acc[who, way, i % 2] = unit(ch, cc, h, way, i)

            @pl.when(step < 2)
            def _():
                part(way, i).start()
            return carry
        lax.fori_loop(0, 4, one, 0)

    enter((right, left, partner))
    loaded = set()

    def ensure(ch):
        if ch not in loaded:
            loaded.add(ch)
            load(ch).wait()

    for i in range(steps):
        k = 3 - (i + 1) // 2
        chans = (2 * k, 2 * k - 1)
        for ch in chans:
            ensure(ch)
        for way in range(2):
            if i < 2:
                load_head(way, i).wait()
            else:
                ring(way, i - 2).wait_send()
                part(way, i - 2).wait_send()
        units(i, chans, (i % 2, 1 - i % 2))
        for way in range(2):
            part(way, i).wait_recv()
            if i >= 2:
                ring(way, i - 2).wait_recv()
                acc[0, way, i % 2] = acc[0, way, i % 2] + part_in[way, i] + ring_in[way, i - 2]
            else:
                acc[0, way, i % 2] = acc[0, way, i % 2] + part_in[way, i]
            ring(way, i).start()
    ensure(0)
    for way in range(2):
        ring(way, steps - 2).wait_send()
        part(way, steps - 2).wait_send()
    units(steps, (0, 0), (0, 1))
    for h in range(2):
        part(h, steps).wait_recv()
        ring(1 - h, steps - 2).wait_recv()
        cols = slice(h * half, (h + 1) * half)
        acc[0, h, steps % 2] = (acc[0, h, steps % 2] + part_in[h, steps] + ring_in[1 - h, steps - 2]
                                + shared_ref[:, cols] + hidden_ref[:, cols].astype(F32))
    for h in range(2):
        ring(h, steps - 1).wait_recv()
        cols = slice(h * half, (h + 1) * half)
        out_ref[:, cols] = (acc[0, h, steps % 2] + ring_in[h, steps - 1]).astype(BF16)
    for way in range(2):
        ring(way, steps - 1).wait_send()
        part(way, steps - 1).wait_send()
        part(way, steps).wait_send()


WINDOW = 48


def solution(mesh):
    group_size = mesh.shape['ep']
    chips = group_size // CORES

    def local_step(hidden, norm_gain, router_w, topk_idx, w_gate, w_up, w_down, shared_gate, shared_up, shared_down):
        tokens, hidden_size = hidden.shape
        num_experts = router_w.shape[1]
        local_count, _, ff = w_gate.shape
        capacity = 3 * tokens * topk_idx.shape[1] // (2 * num_experts)
        slots = (CORES * capacity + 15) // 16 * 16
        before = jnp.triu(jnp.ones((tokens, tokens), BF16), 1)
        hbm = pl.BlockSpec(memory_space=pl.ANY)
        vmem = pl.BlockSpec(memory_space=pltpu.VMEM)
        dma = pltpu.SemaphoreType.DMA
        expert_out, heads, sides, shared_out = pl.pallas_call(
            functools.partial(gather_kernel, group_size, capacity, slots),
            in_specs=[hbm, vmem, vmem, vmem, vmem] + [hbm] * 6,
            out_specs=(hbm, hbm, vmem, vmem),
            out_shape=(jax.ShapeDtypeStruct((local_count, chips, slots, hidden_size), BF16),
                       jax.ShapeDtypeStruct((2, 2, local_count, slots, hidden_size // 2), BF16),
                       jax.ShapeDtypeStruct((chips, CORES, 16, tokens), F32),
                       jax.ShapeDtypeStruct((tokens, hidden_size), F32)),
            scratch_shapes=[
                pltpu.VMEM((chips, CORES * tokens, hidden_size), BF16),
                pltpu.VMEM((chips + 1, CORES, 16, tokens), F32),
                pltpu.VMEM((local_count, 3, slots, hidden_size), BF16),
                pltpu.VMEM((local_count * slots, CORES * tokens), BF16),
                pltpu.VMEM((2, hidden_size, ff), BF16),
                pltpu.VMEM((2, hidden_size, ff), BF16),
                pltpu.VMEM((ff, hidden_size), BF16),
                dma((2, 7)), dma((2, 7)), dma((2, 7)), dma((2, 7)),
                dma((2, 4)), dma((2, 4)), dma((2, 4)), dma((2, 4)),
                dma((2,)), dma((2,)), dma((2, 2, local_count)), dma((2, 2, local_count)),
                dma((1,)), dma((5,)), dma((local_count,)),
            ],
            compiler_params=pltpu.CompilerParams(collective_id=0, has_side_effects=True, vmem_limit_bytes=VMEM_LIMIT),
            name='gather_experts',
        )(hidden, norm_gain[None, :], router_w.T, topk_idx.T, before, shared_gate, shared_up, shared_down, w_gate, w_up, w_down)
        return pl.pallas_call(
            functools.partial(scatter_kernel, group_size, capacity),
            in_specs=[hbm, hbm, vmem, vmem, vmem, vmem],
            out_specs=vmem,
            out_shape=jax.ShapeDtypeStruct((tokens, hidden_size), BF16),
            scratch_shapes=[
                pltpu.VMEM((local_count, chips, slots, hidden_size), BF16),
                pltpu.VMEM((2, 2, local_count, slots, hidden_size // 2), BF16),
                pltpu.VMEM((2, 2, 2, tokens, hidden_size // 2), F32),
                pltpu.VMEM((2, 6, tokens, hidden_size // 2), F32),
                pltpu.VMEM((2, 5, tokens, hidden_size // 2), F32),
                dma((chips,)), dma((2, 2)), dma((2, 5)), dma((2, 5)), dma((2, 6)), dma((2, 6)),
            ],
            compiler_params=pltpu.CompilerParams(collective_id=1, has_side_effects=True, vmem_limit_bytes=VMEM_LIMIT),
            name='combine_scatter',
        )(expert_out, heads, sides, before, hidden, shared_out)

    token_spec = P(('dp', 'ep'), None)
    expert_spec = P('ep', None, None)
    return jax.shard_map(
        local_step,
        mesh=mesh,
        in_specs=(token_spec, P(None), P(None, None), token_spec, expert_spec, expert_spec, expert_spec,
                  P(None, None), P(None, None), P(None, None)),
        out_specs=token_spec,
        check_vma=False,
    )
```

```python
import functools

import jax
import jax.numpy as jnp
from jax import lax
from jax.experimental import pallas as pl
from jax.experimental.pallas import tpu as pltpu
from jax.sharding import PartitionSpec as P

NORM_EPS = 1e-6
CORES = 2
VMEM_LIMIT = 67043328
F32 = jnp.float32
BF16 = jnp.bfloat16


def slots_of(side, first_expert, local_count, before):
    ids, weights = side[0:8], side[8:16]
    chosen, picked = [], []
    for e in range(8):
        hit = ids == (first_expert + e).astype(F32)
        chosen.append(jnp.sum(jnp.where(hit, 1.0, 0.0), axis=0, keepdims=True))
        picked.append(jnp.sum(jnp.where(hit, weights, 0.0), axis=0, keepdims=True))
    chosen = jnp.concatenate(chosen, axis=0)
    rank = jnp.dot(chosen.astype(BF16), before, preferred_element_type=F32)
    slot = jnp.where(chosen > 0.5, rank, -1000.0)
    return [slot[e:e + 1] for e in range(local_count)], picked[:local_count]


def place_of(group_size):
    chips = group_size // CORES
    me = lax.axis_index('ep')
    chip, core = me // CORES, me % CORES
    right = (chip + 1) % chips * CORES + core
    left = (chip + chips - 1) % chips * CORES + core
    return me, chip, core, right, left, chip * CORES + (1 - core)


def enter(neighbours):
    barrier = pltpu.get_barrier_semaphore()
    for device in neighbours:
        pl.semaphore_signal(barrier, inc=1, device_id={'ep': device}, device_id_type=pl.DeviceIdType.MESH)
    pl.semaphore_wait(barrier, len(neighbours))


def remote(src, dst, send_sem, recv_sem, device):
    return pltpu.make_async_remote_copy(src_ref=src, dst_ref=dst, send_sem=send_sem, recv_sem=recv_sem,
                                        device_id={'ep': device}, device_id_type=pl.DeviceIdType.MESH)


def gather_kernel(group_size, capacity, slots, hidden_hbm, gain_ref, router_ref, idx_ref, before_ref,
                  sgate, sup, sdown, wgate, wup, wdown,
                  out_hbm, peer_hbm, head_hbm, side_out, shared_ref,
                  rows, sides, x_ref, pick, gate_buf, up_buf, down_buf,
                  ring_s, ring_r, part_s, part_r, tring_s, tring_r, tpart_s, tpart_r, own_s, own_r,
                  head_s, head_r, peer_s, peer_r, load_sem, w_sem, out_sem):
    me, _, core, right, left, partner = place_of(group_size)
    local_count, hidden_size, ff = wgate.shape
    tokens = hidden_hbm.shape[0]
    half = tokens // 2
    half_cols = hidden_size // 2
    last = group_size // CORES - 1
    mine = pl.multiple_of(core * tokens, tokens)
    other = pl.multiple_of((1 - core) * tokens, tokens)

    def order(way, n):
        return min(2 * n + 1 + way, last)

    def piece(way, i, base):
        r = i % 2 if way == 0 else 1 - i % 2
        return rows.at[order(way, i // 2), pl.ds(pl.multiple_of(base + r * half, half), half)]

    def ring(way, i):
        n = i // 2
        r = i % 2 if way == 0 else 1 - i % 2
        src = 0 if n == 0 else order(way, n - 1)
        return remote(rows.at[src, pl.ds(pl.multiple_of(mine + r * half, half), half)], piece(way, i, mine),
                      ring_s.at[way, i], ring_r.at[way, i], right if way == 0 else left)

    def part(way, i, base):
        return remote(piece(way, i, base), piece(way, i, base), part_s.at[way, i], part_r.at[way, i], partner)

    def tring(way, n):
        src = 0 if n == 0 else 2 * (n - 1) + 1 + way
        return remote(sides.at[src, core], sides.at[2 * n + 1 + way, core],
                      tring_s.at[way, n], tring_r.at[way, n], right if way == 0 else left)

    def tpart(way, n, who):
        place = sides.at[2 * n + 1 + way, who]
        return remote(place, place, tpart_s.at[way, n], tpart_r.at[way, n], partner)

    def own_part(base):
        place = rows.at[0, pl.ds(base, tokens)]
        return remote(place, place, own_s.at[0], own_r.at[0], partner)

    def own_tpart(who):
        place = sides.at[0, who]
        return remote(place, place, own_s.at[1], own_r.at[1], partner)

    sends = 7

    def send(i):
        for way in range(2):
            ring(way, i).start()
            if i % 2 == 0 and i > 0:
                tring(way, i // 2).start()

    def service(i):
        for way in range(2):
            ring(way, i).wait_recv()
            if i % 2 == 0:
                tring(way, i // 2).wait_recv()
        if i + 2 < sends:
            send(i + 2)
        for way in range(2):
            part(way, i, mine).start()
            if i % 2 == 0:
                tpart(way, i // 2, core).start()

    def partner_arrived(i):
        for way in range(2):
            part(way, i, other).wait_recv()
            if i % 2 == 0:
                tpart(way, i // 2, 1 - core).wait_recv()

    beside = (right - core, left - core)

    def head(way, step, e, cc, source):
        chip_row, cols = (((2, 0), (1, 1)), ((2, 1), (0, 0)))[way][step]
        return remote(x_ref.at[e, chip_row, pl.ds(cc * HEAD_START, HEAD_ROWS), cols * half_cols:(cols + 1) * half_cols],
                      head_hbm.at[way, step, source, e], head_s.at[way, step, e, cc], head_r.at[way, step, e, source],
                      beside[way] + cc)

    def send_heads(step, e):
        for way in range(2):
            for cc in range(CORES):
                head(way, step, e, cc, core).start()

    def peer(turn, first, count, e):
        return remote(x_ref.at[e, 0:count], peer_hbm.at[e, pl.ds(first, count)], peer_s.at[turn, e], peer_r.at[turn, e], partner)

    load_rows = pltpu.make_async_copy(hidden_hbm, rows.at[0, pl.ds(mine, tokens)], load_sem.at[0])
    load_rows.start()

    def normalise():
        block = 32

        def one(i, carry):
            place = pl.ds(pl.multiple_of(mine + i * block, block), block)
            x = rows[0, place, :].astype(F32)
            inv_rms = lax.rsqrt(jnp.mean(x * x, axis=-1, keepdims=True) + NORM_EPS)
            rows[0, place, :] = (x * inv_rms * gain_ref[...]).astype(BF16)
            return carry
        lax.fori_loop(0, tokens // block, one, 0)

    def route():
        x = rows[0, pl.ds(mine, tokens), :]
        logits = lax.dot_general(router_ref[...], x, (((1,), (1,)), ((), ())), preferred_element_type=F32)
        top = jnp.exp(logits - jnp.max(logits, axis=0, keepdims=True))
        probs = top / jnp.sum(top, axis=0, keepdims=True)
        experts_id = lax.broadcasted_iota(jnp.int32, probs.shape, 0)
        sides[0, core] = jnp.full((16, tokens), -1.0, F32)
        for j in range(idx_ref.shape[0]):
            idx = idx_ref[j:j + 1, :]
            sides[0, core, j:j + 1, :] = idx.astype(F32)
            sides[0, core, 8 + j:9 + j, :] = jnp.sum(jnp.where(experts_id == idx, probs, 0.0), axis=0, keepdims=True)

    def gate_copies(slot, gate, up):
        return (pltpu.make_async_copy(gate, gate_buf.at[slot], w_sem.at[slot]),
                pltpu.make_async_copy(up, up_buf.at[slot], w_sem.at[2 + slot]))

    def start_gate(slot, gate, up):
        for copy in gate_copies(slot, gate, up):
            copy.start()

    def down_copy(down):
        return pltpu.make_async_copy(down, down_buf, w_sem.at[4])

    def shared_cols(ref, i):
        return ref.at[:, pl.ds(pl.multiple_of(i * ff, 128), ff)]

    start_gate(0, shared_cols(sgate, 0), shared_cols(sup, 0))
    enter([device + cc for device in beside for cc in range(CORES)] + [partner])
    load_rows.wait()
    normalise()
    send(0)
    send(1)
    own_part(mine).start()
    route()
    for way in range(2):
        tring(way, 0).start()
    own_tpart(core).start()

    def activate(x, slot, fresh=True):
        if fresh:
            for copy in gate_copies(slot, wgate.at[0], wup.at[0]):
                copy.wait()
        gate_out = jnp.dot(x, gate_buf[slot], preferred_element_type=F32)
        up_out = jnp.dot(x, up_buf[slot], preferred_element_type=F32)
        return (jax.nn.silu(gate_out) * up_out).astype(BF16)

    def project(act, fresh=True):
        if fresh:
            down_copy(wdown.at[0]).wait()
        return jnp.dot(act, down_buf[...], preferred_element_type=F32)

    shared_parts = sgate.shape[1] // ff

    def shared(i, carry):
        slot = i % 2
        down_copy(sdown.at[pl.ds(pl.multiple_of(i * ff, 128), ff)]).start()

        @pl.when(i < shared_parts - 1)
        def _():
            start_gate(1 - slot, shared_cols(sgate, i + 1), shared_cols(sup, i + 1))

        @pl.when(i == shared_parts - 1)
        def _():
            start_gate(1 - slot, wgate.at[0], wup.at[0])
        shared_ref[...] += project(activate(rows[0, pl.ds(mine, tokens), :], slot))
        return carry

    shared_ref[...] = jnp.zeros_like(shared_ref)
    lax.fori_loop(0, shared_parts, shared, 0)

    def dispatch(base, start, count):
        def one(ch, carry):
            for cc in range(CORES):
                slot, _ = slots_of(sides[ch, cc], me * local_count, local_count, before_ref[...])
                row_id = lax.broadcasted_iota(jnp.int32, (slots, tokens), 0).astype(F32)
                for e in range(local_count):
                    hit = row_id == slot[e] + float(capacity * cc)
                    pick[e * slots:(e + 1) * slots, cc * tokens:(cc + 1) * tokens] = jnp.where(hit, 1.0, 0.0).astype(BF16)
            step = min(512, hidden_size)
            for n in range(0, hidden_size, step):
                got = jnp.dot(pick[...], rows[ch, :, n:n + step], preferred_element_type=F32).astype(BF16)
                for e in range(local_count):
                    x_ref[e, ch - base, :, n:n + step] = got[e * slots:(e + 1) * slots]
            return carry
        lax.fori_loop(start, start + count, one, 0)

    def stage_copy(e, first, count):
        return pltpu.make_async_copy(x_ref.at[e, 0:count], out_hbm.at[e, pl.ds(first, count)], out_sem.at[e])

    def start_next(e, slot):
        down_copy(wdown.at[e]).start()
        following = (e + 1) % local_count
        start_gate(1 - slot, wgate.at[following], wup.at[following])

    def mlp(e, slot, begin, count, fresh):
        x = x_ref[e, begin:begin + count].reshape(count * slots, hidden_size)
        out = project(activate(x, slot, fresh), fresh).astype(BF16)
        x_ref[e, begin:begin + count] = out.reshape(count, slots, hidden_size)

    def put(turn, first, count, e):
        stage_copy(e, first, count).start()
        peer(turn, first, count, e).start()

    def experts(turn, first, count, middle):
        def one(e, carry):
            @pl.when(e == local_count // 2)
            def _():
                service(middle)
            start_next(e, e % 2)
            mlp(e, e % 2, 0, count, True)
            put(turn, first, count, e)
            return carry
        lax.fori_loop(0, local_count, one, 0)

    def last_experts(turn, first, count):
        start_next(0, 0)
        mlp(0, 0, 0, count - 1, True)
        send_heads(1, 0)
        service(6)
        partner_arrived(6)
        dispatch(first, first + count - 1, 1)
        mlp(0, 0, count - 1, 1, False)
        send_heads(0, 0)
        put(turn, first, count, 0)

        def one(e, carry):
            slot = e % 2
            down_copy(wdown.at[e]).start()

            @pl.when(e < local_count - 1)
            def _():
                start_gate(1 - slot, wgate.at[e + 1], wup.at[e + 1])
            mlp(e, slot, 0, count, True)
            send_heads(1, e)
            send_heads(0, e)
            put(turn, first, count, e)
            return carry
        lax.fori_loop(1, local_count, one, 0)

    def finish(turn, first, count):
        for e in range(local_count):
            stage_copy(e, first, count).wait()
            peer(turn, first, count, e).wait_send()

    service(0)
    own_part(other).wait_recv()
    own_tpart(1 - core).wait_recv()
    dispatch(0, 0, 1)
    service(1)
    partner_arrived(0)
    partner_arrived(1)
    dispatch(0, 1, 2)
    experts(0, 0, 3, 2)
    finish(0, 0, 3)
    service(3)
    partner_arrived(2)
    partner_arrived(3)
    dispatch(3, 3, 2)
    experts(1, 3, 2, 4)
    finish(1, 3, 2)
    service(5)
    partner_arrived(4)
    partner_arrived(5)
    dispatch(5, 5, 2)
    last_experts(2, 5, 3)
    finish(2, 5, 3)
    side_out[...] = sides[0:group_size // CORES]
    for way in range(2):
        for i in range(sends):
            ring(way, i).wait_send()
            part(way, i, mine).wait_send()
            if i % 2 == 0:
                tring(way, i // 2).wait_send()
                tpart(way, i // 2, core).wait_send()
    own_part(mine).wait_send()
    own_tpart(core).wait_send()
    for turn, (first, count) in enumerate(((0, 3), (3, 2), (5, 3))):
        for e in range(local_count):
            peer(turn, first, count, e).wait_recv()

    def settle(e, carry):
        for step in range(2):
            for way in range(2):
                for cc in range(CORES):
                    head(way, step, e, cc, cc).wait_recv()
                    head(way, step, e, cc, cc).wait_send()
        return carry
    lax.fori_loop(0, local_count, settle, 0)


def scatter_kernel(group_size, capacity, rows_hbm, peer_hbm, head_hbm, side_ref, before_ref, hidden_ref, shared_ref, out_ref,
                   rows, heads, acc, ring_in, load_sem, head_sem, ring_s, ring_r):
    _, chip, core, right, left, _ = place_of(group_size)
    _, local_count, chips, _, hidden_size = rows.shape
    tokens = hidden_ref.shape[0]
    half = hidden_size // 2
    last = chips - 1
    steps = 5
    window = pl.ds(pl.multiple_of(core * HEAD_START, HEAD_START), WINDOW)

    def load(ch):
        return (pltpu.make_async_copy(rows_hbm.at[:, ch, window], rows.at[core, :, ch], load_sem.at[0, ch]),
                pltpu.make_async_copy(peer_hbm.at[:, ch, window], rows.at[1 - core, :, ch], load_sem.at[1, ch]))

    def load_head(way, i):
        return pltpu.make_async_copy(head_hbm.at[way, i], heads.at[way, i, :, :, 0:HEAD_ROWS], head_sem.at[way, i])

    for i in range(2):
        for way in range(2):
            load_head(way, i).start()
            for copy in load((last - 1, last - 2, 4, 3)[2 * i + way]):
                copy.start()
    for ch in (2, 1, 0):
        for copy in load(ch):
            copy.start()
    heads[:, :, :, :, HEAD_ROWS:WINDOW, :] = jnp.zeros((2, 2, CORES, local_count, WINDOW - HEAD_ROWS, half), BF16)

    def ring(way, i):
        return remote(acc.at[way, i % 2], ring_in.at[way, i], ring_s.at[way, i], ring_r.at[way, i],
                      right if way == 0 else left)

    def mix_of(ch, from_chip):
        count = CORES * local_count
        slot, weight = slots_of(side_ref[ch, core], from_chip * count, count, before_ref[...])
        row_id = lax.broadcasted_iota(jnp.int32, (WINDOW, tokens), 0).astype(F32)
        shift = (core * (capacity - HEAD_START)).astype(F32)
        return [jnp.where(row_id == slot[e] + shift, weight[e], 0.0) for e in range(count)]

    def unit(ch, h, way, i):
        col = pl.multiple_of(h * half, half)
        mix = mix_of(ch, chip)
        picked = [rows[cc, e, ch, :, pl.ds(col, half)] for cc in range(CORES) for e in range(local_count)]
        if i < 2:
            mix += mix_of(ch, (left + way * (right - left)) // CORES)
            picked += [heads[way, i, cc, e] for cc in range(CORES) for e in range(local_count)]
        mix = jnp.concatenate(mix, axis=0)
        picked = jnp.concatenate(picked, axis=0)
        high = mix.astype(BF16)
        rest = mix - high.astype(F32)
        mid = rest.astype(BF16)
        low = (rest - mid.astype(F32)).astype(BF16)
        total = jnp.dot(high.T, picked, preferred_element_type=F32)
        total += jnp.dot(mid.T, picked, preferred_element_type=F32)
        return total + jnp.dot(low.T, picked, preferred_element_type=F32)

    def units(i, chans, halves):
        def one(way, carry):
            ch = chans[0] + way * (chans[1] - chans[0])
            h = halves[0] + way * (halves[1] - halves[0])
            acc[way, i % 2] = unit(ch, h, way, i)
            return carry
        lax.fori_loop(0, 2, one, 0)

    enter((right, left))
    loaded = set()

    def ensure(ch):
        if ch not in loaded:
            loaded.add(ch)
            for copy in load(ch):
                copy.wait()

    for i in range(steps):
        k = 3 - (i + 1) // 2
        chans = (2 * k, 2 * k - 1)
        for ch in chans:
            ensure(ch)
        for way in range(2):
            if i < 2:
                load_head(way, i).wait()
            else:
                ring(way, i - 2).wait_send()
        units(i, chans, (i % 2, 1 - i % 2))
        for way in range(2):
            if i >= 2:
                ring(way, i - 2).wait_recv()
                acc[way, i % 2] = acc[way, i % 2] + ring_in[way, i - 2]
            ring(way, i).start()
    ensure(0)
    for way in range(2):
        ring(way, steps - 2).wait_send()
    units(steps, (0, 0), (0, 1))
    for h in range(2):
        ring(1 - h, steps - 2).wait_recv()
        cols = slice(h * half, (h + 1) * half)
        acc[h, steps % 2] = (acc[h, steps % 2] + ring_in[1 - h, steps - 2]
                             + shared_ref[:, cols] + hidden_ref[:, cols].astype(F32))
    for h in range(2):
        ring(h, steps - 1).wait_recv()
        cols = slice(h * half, (h + 1) * half)
        out_ref[:, cols] = (acc[h, steps % 2] + ring_in[h, steps - 1]).astype(BF16)
    for way in range(2):
        ring(way, steps - 1).wait_send()


WINDOW = 48
HEAD_START = 32
HEAD_ROWS = 40


def solution(mesh):
    group_size = mesh.shape['ep']
    chips = group_size // CORES

    def local_step(hidden, norm_gain, router_w, topk_idx, w_gate, w_up, w_down, shared_gate, shared_up, shared_down):
        tokens, hidden_size = hidden.shape
        num_experts = router_w.shape[1]
        local_count, _, ff = w_gate.shape
        capacity = 3 * tokens * topk_idx.shape[1] // (2 * num_experts)
        slots = (CORES * capacity + 15) // 16 * 16
        before = jnp.triu(jnp.ones((tokens, tokens), BF16), 1)
        hbm = pl.BlockSpec(memory_space=pl.ANY)
        vmem = pl.BlockSpec(memory_space=pltpu.VMEM)
        dma = pltpu.SemaphoreType.DMA
        expert_out, peer_out, heads, sides, shared_out = pl.pallas_call(
            functools.partial(gather_kernel, group_size, capacity, slots),
            in_specs=[hbm, vmem, vmem, vmem, vmem] + [hbm] * 6,
            out_specs=(hbm, hbm, hbm, vmem, vmem),
            out_shape=(jax.ShapeDtypeStruct((local_count, chips, slots, hidden_size), BF16),
                       jax.ShapeDtypeStruct((local_count, chips, slots, hidden_size), BF16),
                       jax.ShapeDtypeStruct((2, 2, CORES, local_count, HEAD_ROWS, hidden_size // 2), BF16),
                       jax.ShapeDtypeStruct((chips, CORES, 16, tokens), F32),
                       jax.ShapeDtypeStruct((tokens, hidden_size), F32)),
            scratch_shapes=[
                pltpu.VMEM((chips, CORES * tokens, hidden_size), BF16),
                pltpu.VMEM((chips + 1, CORES, 16, tokens), F32),
                pltpu.VMEM((local_count, 3, slots, hidden_size), BF16),
                pltpu.VMEM((local_count * slots, CORES * tokens), BF16),
                pltpu.VMEM((2, hidden_size, ff), BF16),
                pltpu.VMEM((2, hidden_size, ff), BF16),
                pltpu.VMEM((ff, hidden_size), BF16),
                dma((2, 7)), dma((2, 7)), dma((2, 7)), dma((2, 7)),
                dma((2, 4)), dma((2, 4)), dma((2, 4)), dma((2, 4)),
                dma((2,)), dma((2,)), dma((2, 2, local_count, CORES)), dma((2, 2, local_count, CORES)),
                dma((3, local_count)), dma((3, local_count)),
                dma((1,)), dma((5,)), dma((local_count,)),
            ],
            compiler_params=pltpu.CompilerParams(collective_id=0, has_side_effects=True, vmem_limit_bytes=VMEM_LIMIT),
            name='gather_experts',
        )(hidden, norm_gain[None, :], router_w.T, topk_idx.T, before, shared_gate, shared_up, shared_down, w_gate, w_up, w_down)
        return pl.pallas_call(
            functools.partial(scatter_kernel, group_size, capacity),
            in_specs=[hbm, hbm, hbm, vmem, vmem, vmem, vmem],
            out_specs=vmem,
            out_shape=jax.ShapeDtypeStruct((tokens, hidden_size), BF16),
            scratch_shapes=[
                pltpu.VMEM((CORES, local_count, chips, WINDOW, hidden_size), BF16),
                pltpu.VMEM((2, 2, CORES, local_count, WINDOW, hidden_size // 2), BF16),
                pltpu.VMEM((2, 2, tokens, hidden_size // 2), F32),
                pltpu.VMEM((2, 5, tokens, hidden_size // 2), F32),
                dma((CORES, chips)), dma((2, 2)), dma((2, 5)), dma((2, 5)),
            ],
            compiler_params=pltpu.CompilerParams(collective_id=1, has_side_effects=True, vmem_limit_bytes=VMEM_LIMIT),
            name='combine_scatter',
        )(expert_out, peer_out, heads, sides, before, hidden, shared_out)

    token_spec = P(('dp', 'ep'), None)
    expert_spec = P('ep', None, None)
    return jax.shard_map(
        local_step,
        mesh=mesh,
        in_specs=(token_spec, P(None), P(None, None), token_spec, expert_spec, expert_spec, expert_spec,
                  P(None, None), P(None, None), P(None, None)),
        out_specs=token_spec,
        check_vma=False,
    )
```

```python
import functools

import jax
import jax.numpy as jnp
from jax import lax
from jax.experimental import pallas as pl
from jax.experimental.pallas import tpu as pltpu
from jax.sharding import PartitionSpec as P

NORM_EPS = 1e-6
CORES = 2
VMEM_LIMIT = 67043328
F32 = jnp.float32
BF16 = jnp.bfloat16


def slots_of(side, first_expert, local_count, before):
    ids, weights = side[0:8], side[8:16]
    chosen, picked = [], []
    for e in range(8):
        hit = ids == (first_expert + e).astype(F32)
        chosen.append(jnp.sum(jnp.where(hit, 1.0, 0.0), axis=0, keepdims=True))
        picked.append(jnp.sum(jnp.where(hit, weights, 0.0), axis=0, keepdims=True))
    chosen = jnp.concatenate(chosen, axis=0)
    rank = jnp.dot(chosen.astype(BF16), before, preferred_element_type=F32)
    slot = jnp.where(chosen > 0.5, rank, -1000.0)
    return [slot[e:e + 1] for e in range(local_count)], picked[:local_count]


def place_of(group_size):
    chips = group_size // CORES
    me = lax.axis_index('ep')
    chip, core = me // CORES, me % CORES
    right = (chip + 1) % chips * CORES + core
    left = (chip + chips - 1) % chips * CORES + core
    return me, chip, core, right, left, chip * CORES + (1 - core)


def announce(neighbours):
    for device in neighbours:
        pl.semaphore_signal(pltpu.get_barrier_semaphore(), inc=1, device_id={'ep': device},
                            device_id_type=pl.DeviceIdType.MESH)


def meet(neighbours):
    pl.semaphore_wait(pltpu.get_barrier_semaphore(), len(neighbours))


def fill_before(before):
    row = lax.broadcasted_iota(jnp.int32, before.shape, 0)
    col = lax.broadcasted_iota(jnp.int32, before.shape, 1)
    before[...] = jnp.where(row < col, 1.0, 0.0).astype(BF16)


def remote(src, dst, send_sem, recv_sem, device):
    return pltpu.make_async_remote_copy(src_ref=src, dst_ref=dst, send_sem=send_sem, recv_sem=recv_sem,
                                        device_id={'ep': device}, device_id_type=pl.DeviceIdType.MESH)


def gather_kernel(group_size, capacity, slots, hidden_hbm, gain_ref, router_ref, idx_ref,
                  sgate, sup, sdown, wgate, wup, wdown,
                  out_hbm, peer_hbm, head_hbm, side_out, shared_ref,
                  before_ref, rows, sides, x_ref, pick, gate_buf, up_buf, down_buf,
                  ring_s, ring_r, part_s, part_r, tring_s, tring_r, tpart_s, tpart_r, own_s, own_r,
                  head_s, head_r, peer_s, peer_r, load_sem, w_sem, out_sem):
    me, _, core, right, left, partner = place_of(group_size)
    local_count, hidden_size, ff = wgate.shape
    tokens = hidden_hbm.shape[0]
    half = tokens // 2
    half_cols = hidden_size // 2
    last = group_size // CORES - 1
    mine = pl.multiple_of(core * tokens, tokens)
    other = pl.multiple_of((1 - core) * tokens, tokens)

    def order(way, n):
        return min(2 * n + 1 + way, last)

    def piece(way, i, base):
        r = i % 2 if way == 0 else 1 - i % 2
        return rows.at[order(way, i // 2), pl.ds(pl.multiple_of(base + r * half, half), half)]

    def ring(way, i):
        n = i // 2
        r = i % 2 if way == 0 else 1 - i % 2
        src = 0 if n == 0 else order(way, n - 1)
        return remote(rows.at[src, pl.ds(pl.multiple_of(mine + r * half, half), half)], piece(way, i, mine),
                      ring_s.at[way, i], ring_r.at[way, i], right if way == 0 else left)

    def part(way, i, base):
        return remote(piece(way, i, base), piece(way, i, base), part_s.at[way, i], part_r.at[way, i], partner)

    def tring(way, n):
        src = 0 if n == 0 else 2 * (n - 1) + 1 + way
        return remote(sides.at[src, core], sides.at[2 * n + 1 + way, core],
                      tring_s.at[way, n], tring_r.at[way, n], right if way == 0 else left)

    def tpart(way, n, who):
        place = sides.at[2 * n + 1 + way, who]
        return remote(place, place, tpart_s.at[way, n], tpart_r.at[way, n], partner)

    def own_part(base):
        place = rows.at[0, pl.ds(base, tokens)]
        return remote(place, place, own_s.at[0], own_r.at[0], partner)

    def own_tpart(who):
        place = sides.at[0, who]
        return remote(place, place, own_s.at[1], own_r.at[1], partner)

    sends = 7

    def send(i):
        for way in range(2):
            ring(way, i).start()
            if i % 2 == 0 and i > 0:
                tring(way, i // 2).start()

    def service(i):
        for way in range(2):
            ring(way, i).wait_recv()
            if i % 2 == 0:
                tring(way, i // 2).wait_recv()
        if i + 2 < sends:
            send(i + 2)
        for way in range(2):
            part(way, i, mine).start()
            if i % 2 == 0:
                tpart(way, i // 2, core).start()

    def partner_arrived(i):
        for way in range(2):
            part(way, i, other).wait_recv()
            if i % 2 == 0:
                tpart(way, i // 2, 1 - core).wait_recv()

    beside = (right - core, left - core)

    def head(way, step, e, cc, source):
        chip_row, cols = (((2, 0), (1, 1)), ((2, 1), (0, 0)))[way][step]
        return remote(x_ref.at[e, chip_row, pl.ds(cc * HEAD_START, HEAD_ROWS), cols * half_cols:(cols + 1) * half_cols],
                      head_hbm.at[way, step, source, e], head_s.at[way, step, e, cc], head_r.at[way, step, e, source],
                      beside[way] + cc)

    def send_heads(step, e):
        for way in range(2):
            for cc in range(CORES):
                head(way, step, e, cc, core).start()

    def peer(turn, first, count, e):
        return remote(x_ref.at[e, 0:count], peer_hbm.at[e, pl.ds(first, count)], peer_s.at[turn, e], peer_r.at[turn, e], partner)

    load_rows = pltpu.make_async_copy(hidden_hbm, rows.at[0, pl.ds(mine, tokens)], load_sem.at[0])
    load_rows.start()

    def normalise():
        block = 32

        def one(i, carry):
            place = pl.ds(pl.multiple_of(mine + i * block, block), block)
            x = rows[0, place, :].astype(F32)
            inv_rms = lax.rsqrt(jnp.mean(x * x, axis=-1, keepdims=True) + NORM_EPS)
            rows[0, place, :] = (x * inv_rms * gain_ref[...]).astype(BF16)
            return carry
        lax.fori_loop(0, tokens // block, one, 0)

    def route():
        x = rows[0, pl.ds(mine, tokens), :]
        logits = lax.dot_general(router_ref[...], x, (((1,), (1,)), ((), ())), preferred_element_type=F32)
        top = jnp.exp(logits - jnp.max(logits, axis=0, keepdims=True))
        probs = top / jnp.sum(top, axis=0, keepdims=True)
        experts_id = lax.broadcasted_iota(jnp.int32, probs.shape, 0)
        sides[0, core] = jnp.full((16, tokens), -1.0, F32)
        for j in range(idx_ref.shape[0]):
            idx = idx_ref[j:j + 1, :]
            sides[0, core, j:j + 1, :] = idx.astype(F32)
            sides[0, core, 8 + j:9 + j, :] = jnp.sum(jnp.where(experts_id == idx, probs, 0.0), axis=0, keepdims=True)

    def gate_copies(slot, gate, up):
        return (pltpu.make_async_copy(gate, gate_buf.at[slot], w_sem.at[slot]),
                pltpu.make_async_copy(up, up_buf.at[slot], w_sem.at[2 + slot]))

    def start_gate(slot, gate, up):
        for copy in gate_copies(slot, gate, up):
            copy.start()

    def down_copy(down):
        return pltpu.make_async_copy(down, down_buf, w_sem.at[4])

    def shared_cols(ref, i):
        return ref.at[:, pl.ds(pl.multiple_of(i * ff, 128), ff)]

    neighbours = [device + cc for device in beside for cc in range(CORES)] + [partner]
    announce(neighbours)
    start_gate(0, shared_cols(sgate, 0), shared_cols(sup, 0))
    down_copy(sdown.at[0:ff]).start()
    start_gate(1, shared_cols(sgate, 1), shared_cols(sup, 1))
    fill_before(before_ref)
    load_rows.wait()
    normalise()
    meet(neighbours)
    send(0)
    send(1)
    own_part(mine).start()
    route()
    for way in range(2):
        tring(way, 0).start()
    own_tpart(core).start()

    def swiglu(x, slot, fresh, next_gate, next_down):
        if fresh:
            for copy in gate_copies(slot, wgate.at[0], wup.at[0]):
                copy.wait()
        gate_out = jnp.dot(x, gate_buf[slot], preferred_element_type=F32)
        up_out = jnp.dot(x, up_buf[slot], preferred_element_type=F32)
        act = (jax.nn.silu(gate_out) * up_out).astype(BF16)
        next_gate()
        if fresh:
            down_copy(wdown.at[0]).wait()
        out = jnp.dot(act, down_buf[...], preferred_element_type=F32)
        next_down()
        return out

    def nothing():
        pass

    shared_parts = 2

    def shared(i, carry):
        slot = i % 2

        def next_down():
            @pl.when(i == 0)
            def _():
                down_copy(sdown.at[ff:2 * ff]).start()

            @pl.when(i == 1)
            def _():
                down_copy(wdown.at[0]).start()
        shared_ref[...] += swiglu(rows[0, pl.ds(mine, tokens), :], slot, True,
                                  lambda: start_gate(slot, wgate.at[i], wup.at[i]), next_down)
        return carry

    shared_ref[...] = jnp.zeros_like(shared_ref)
    lax.fori_loop(0, shared_parts, shared, 0)

    def dispatch(base, start, count):
        def one(ch, carry):
            for cc in range(CORES):
                slot, _ = slots_of(sides[ch, cc], me * local_count, local_count, before_ref[...])
                row_id = lax.broadcasted_iota(jnp.int32, (slots, tokens), 0).astype(F32)
                for e in range(local_count):
                    hit = row_id == slot[e] + float(capacity * cc)
                    pick[e * slots:(e + 1) * slots, cc * tokens:(cc + 1) * tokens] = jnp.where(hit, 1.0, 0.0).astype(BF16)
            step = min(512, hidden_size)
            for n in range(0, hidden_size, step):
                got = jnp.dot(pick[...], rows[ch, :, n:n + step], preferred_element_type=F32).astype(BF16)
                for e in range(local_count):
                    x_ref[e, ch - base, :, n:n + step] = got[e * slots:(e + 1) * slots]
            return carry
        lax.fori_loop(start, start + count, one, 0)

    def stage_copy(e, first, count):
        return pltpu.make_async_copy(x_ref.at[e, 0:count], out_hbm.at[e, pl.ds(first, count)], out_sem.at[e])

    def mlp(e, slot, begin, count, fresh, next_gate, next_down):
        x = x_ref[e, begin:begin + count].reshape(count * slots, hidden_size)
        out = swiglu(x, slot, fresh, next_gate, next_down).astype(BF16)
        x_ref[e, begin:begin + count] = out.reshape(count, slots, hidden_size)

    def gate_after(e, slot):
        ahead = (e + 2) % local_count
        start_gate(slot, wgate.at[ahead], wup.at[ahead])

    def down_after(e):
        down_copy(wdown.at[(e + 1) % local_count]).start()

    def put(turn, first, count, e):
        stage_copy(e, first, count).start()
        peer(turn, first, count, e).start()

    def experts(turn, first, count, middle):
        def one(e, carry):
            @pl.when(e == local_count // 2)
            def _():
                service(middle)
            mlp(e, e % 2, 0, count, True, lambda: gate_after(e, e % 2), lambda: down_after(e))
            put(turn, first, count, e)
            return carry
        lax.fori_loop(0, local_count, one, 0)

    def last_experts(turn, first, count):
        mlp(0, 0, 0, count - 1, True, nothing, nothing)
        send_heads(1, 0)
        service(6)
        partner_arrived(6)
        dispatch(first, first + count - 1, 1)
        mlp(0, 0, count - 1, 1, False, lambda: gate_after(0, 0), lambda: down_after(0))
        send_heads(0, 0)
        put(turn, first, count, 0)

        def one(e, carry):
            def next_gate():
                @pl.when(e < local_count - 2)
                def _():
                    gate_after(e, e % 2)

            def next_down():
                @pl.when(e < local_count - 1)
                def _():
                    down_after(e)
            mlp(e, e % 2, 0, count, True, next_gate, next_down)
            send_heads(1, e)
            send_heads(0, e)
            put(turn, first, count, e)
            return carry
        lax.fori_loop(1, local_count, one, 0)

    def finish(turn, first, count):
        for e in range(local_count):
            stage_copy(e, first, count).wait()
            peer(turn, first, count, e).wait_send()

    service(0)
    own_part(other).wait_recv()
    own_tpart(1 - core).wait_recv()
    dispatch(0, 0, 1)
    service(1)
    partner_arrived(0)
    partner_arrived(1)
    dispatch(0, 1, 2)
    experts(0, 0, 3, 2)
    finish(0, 0, 3)
    service(3)
    partner_arrived(2)
    partner_arrived(3)
    dispatch(3, 3, 2)
    experts(1, 3, 2, 4)
    finish(1, 3, 2)
    service(5)
    partner_arrived(4)
    partner_arrived(5)
    dispatch(5, 5, 2)
    last_experts(2, 5, 3)
    finish(2, 5, 3)
    side_out[...] = sides[0:group_size // CORES]
    for way in range(2):
        for i in range(sends):
            ring(way, i).wait_send()
            part(way, i, mine).wait_send()
            if i % 2 == 0:
                tring(way, i // 2).wait_send()
                tpart(way, i // 2, core).wait_send()
    own_part(mine).wait_send()
    own_tpart(core).wait_send()
    for turn, (first, count) in enumerate(((0, 3), (3, 2), (5, 3))):
        for e in range(local_count):
            peer(turn, first, count, e).wait_recv()

    def settle(e, carry):
        for step in range(2):
            for way in range(2):
                for cc in range(CORES):
                    head(way, step, e, cc, cc).wait_recv()
                    head(way, step, e, cc, cc).wait_send()
        return carry
    lax.fori_loop(0, local_count, settle, 0)


def scatter_kernel(group_size, capacity, rows_hbm, peer_hbm, head_hbm, side_ref, hidden_hbm, shared_hbm, out_ref,
                   before_ref, hidden_ref, shared_ref, rows, heads, acc, ring_in, load_sem, head_sem, base_sem, ring_s, ring_r):
    _, chip, core, right, left, _ = place_of(group_size)
    _, local_count, chips, _, hidden_size = rows.shape
    tokens = hidden_ref.shape[0]
    half = hidden_size // 2
    last = chips - 1
    steps = 5
    window = pl.ds(pl.multiple_of(core * HEAD_START, HEAD_START), WINDOW)

    def load(ch):
        return (pltpu.make_async_copy(rows_hbm.at[:, ch, window], rows.at[core, :, ch], load_sem.at[0, ch]),
                pltpu.make_async_copy(peer_hbm.at[:, ch, window], rows.at[1 - core, :, ch], load_sem.at[1, ch]))

    def load_head(way, i):
        return pltpu.make_async_copy(head_hbm.at[way, i], heads.at[way, i, :, :, 0:HEAD_ROWS], head_sem.at[way, i])

    neighbours = (right, left)
    announce(neighbours)
    for i in range(2):
        for way in range(2):
            load_head(way, i).start()
            for copy in load((last - 1, last - 2, 4, 3)[2 * i + way]):
                copy.start()
    for ch in (2, 1, 0):
        for copy in load(ch):
            copy.start()
    load_base = (pltpu.make_async_copy(hidden_hbm, hidden_ref, base_sem.at[0]),
                 pltpu.make_async_copy(shared_hbm, shared_ref, base_sem.at[1]))
    for copy in load_base:
        copy.start()
    fill_before(before_ref)
    heads[:, :, :, :, HEAD_ROWS:WINDOW, :] = jnp.zeros((2, 2, CORES, local_count, WINDOW - HEAD_ROWS, half), BF16)

    def ring(way, i):
        return remote(acc.at[way, i % 2], ring_in.at[way, i], ring_s.at[way, i], ring_r.at[way, i],
                      right if way == 0 else left)

    def mix_of(ch, from_chip):
        count = CORES * local_count
        slot, weight = slots_of(side_ref[ch, core], from_chip * count, count, before_ref[...])
        row_id = lax.broadcasted_iota(jnp.int32, (WINDOW, tokens), 0).astype(F32)
        shift = (core * (capacity - HEAD_START)).astype(F32)
        return [jnp.where(row_id == slot[e] + shift, weight[e], 0.0) for e in range(count)]

    def unit(ch, h, way, i):
        col = pl.multiple_of(h * half, half)
        mix = mix_of(ch, chip)
        picked = [rows[cc, e, ch, :, pl.ds(col, half)] for cc in range(CORES) for e in range(local_count)]
        if i < 2:
            mix += mix_of(ch, (left + way * (right - left)) // CORES)
            picked += [heads[way, i, cc, e] for cc in range(CORES) for e in range(local_count)]
        mix = jnp.concatenate(mix, axis=0)
        picked = jnp.concatenate(picked, axis=0)
        high = mix.astype(BF16)
        rest = mix - high.astype(F32)
        mid = rest.astype(BF16)
        low = (rest - mid.astype(F32)).astype(BF16)
        total = jnp.dot(high.T, picked, preferred_element_type=F32)
        total += jnp.dot(mid.T, picked, preferred_element_type=F32)
        return total + jnp.dot(low.T, picked, preferred_element_type=F32)

    def units(i, chans, halves):
        def one(way, carry):
            ch = chans[0] + way * (chans[1] - chans[0])
            h = halves[0] + way * (halves[1] - halves[0])
            acc[way, i % 2] = unit(ch, h, way, i)
            return carry
        lax.fori_loop(0, 2, one, 0)

    loaded = set()

    def ensure(ch):
        if ch not in loaded:
            loaded.add(ch)
            for copy in load(ch):
                copy.wait()

    for i in range(steps):
        k = 3 - (i + 1) // 2
        chans = (2 * k, 2 * k - 1)
        for ch in chans:
            ensure(ch)
        for way in range(2):
            if i < 2:
                load_head(way, i).wait()
            else:
                ring(way, i - 2).wait_send()
        units(i, chans, (i % 2, 1 - i % 2))
        if i == 0:
            meet(neighbours)
        for way in range(2):
            if i >= 2:
                ring(way, i - 2).wait_recv()
                acc[way, i % 2] = acc[way, i % 2] + ring_in[way, i - 2]
            ring(way, i).start()
    ensure(0)
    for way in range(2):
        ring(way, steps - 2).wait_send()
    units(steps, (0, 0), (0, 1))
    for copy in load_base:
        copy.wait()
    for h in range(2):
        ring(1 - h, steps - 2).wait_recv()
        cols = slice(h * half, (h + 1) * half)
        acc[h, steps % 2] = (acc[h, steps % 2] + ring_in[1 - h, steps - 2]
                             + shared_ref[:, cols] + hidden_ref[:, cols].astype(F32))
    for h in range(2):
        ring(h, steps - 1).wait_recv()
        cols = slice(h * half, (h + 1) * half)
        out_ref[:, cols] = (acc[h, steps % 2] + ring_in[h, steps - 1]).astype(BF16)
    for way in range(2):
        ring(way, steps - 1).wait_send()


WINDOW = 48
HEAD_START = 32
HEAD_ROWS = 40


def solution(mesh):
    group_size = mesh.shape['ep']
    chips = group_size // CORES

    def local_step(hidden, norm_gain, router_w, topk_idx, w_gate, w_up, w_down, shared_gate, shared_up, shared_down):
        tokens, hidden_size = hidden.shape
        num_experts = router_w.shape[1]
        local_count, _, ff = w_gate.shape
        capacity = 3 * tokens * topk_idx.shape[1] // (2 * num_experts)
        slots = (CORES * capacity + 15) // 16 * 16
        hbm = pl.BlockSpec(memory_space=pl.ANY)
        vmem = pl.BlockSpec(memory_space=pltpu.VMEM)
        dma = pltpu.SemaphoreType.DMA
        expert_out, peer_out, heads, sides, shared_out = pl.pallas_call(
            functools.partial(gather_kernel, group_size, capacity, slots),
            in_specs=[hbm, vmem, vmem, vmem] + [hbm] * 6,
            out_specs=(hbm, hbm, hbm, vmem, vmem),
            out_shape=(jax.ShapeDtypeStruct((local_count, chips, slots, hidden_size), BF16),
                       jax.ShapeDtypeStruct((local_count, chips, slots, hidden_size), BF16),
                       jax.ShapeDtypeStruct((2, 2, CORES, local_count, HEAD_ROWS, hidden_size // 2), BF16),
                       jax.ShapeDtypeStruct((chips, CORES, 16, tokens), F32),
                       jax.ShapeDtypeStruct((tokens, hidden_size), F32)),
            scratch_shapes=[
                pltpu.VMEM((tokens, tokens), BF16),
                pltpu.VMEM((chips, CORES * tokens, hidden_size), BF16),
                pltpu.VMEM((chips + 1, CORES, 16, tokens), F32),
                pltpu.VMEM((local_count, 3, slots, hidden_size), BF16),
                pltpu.VMEM((local_count * slots, CORES * tokens), BF16),
                pltpu.VMEM((2, hidden_size, ff), BF16),
                pltpu.VMEM((2, hidden_size, ff), BF16),
                pltpu.VMEM((ff, hidden_size), BF16),
                dma((2, 7)), dma((2, 7)), dma((2, 7)), dma((2, 7)),
                dma((2, 4)), dma((2, 4)), dma((2, 4)), dma((2, 4)),
                dma((2,)), dma((2,)), dma((2, 2, local_count, CORES)), dma((2, 2, local_count, CORES)),
                dma((3, local_count)), dma((3, local_count)),
                dma((1,)), dma((5,)), dma((local_count,)),
            ],
            compiler_params=pltpu.CompilerParams(collective_id=0, has_side_effects=True, vmem_limit_bytes=VMEM_LIMIT),
            name='gather_experts',
        )(hidden, norm_gain[None, :], router_w.T, topk_idx.T, shared_gate, shared_up, shared_down, w_gate, w_up, w_down)
        return pl.pallas_call(
            functools.partial(scatter_kernel, group_size, capacity),
            in_specs=[hbm, hbm, hbm, vmem, hbm, hbm],
            out_specs=vmem,
            out_shape=jax.ShapeDtypeStruct((tokens, hidden_size), BF16),
            scratch_shapes=[
                pltpu.VMEM((tokens, tokens), BF16),
                pltpu.VMEM((tokens, hidden_size), BF16),
                pltpu.VMEM((tokens, hidden_size), F32),
                pltpu.VMEM((CORES, local_count, chips, WINDOW, hidden_size), BF16),
                pltpu.VMEM((2, 2, CORES, local_count, WINDOW, hidden_size // 2), BF16),
                pltpu.VMEM((2, 2, tokens, hidden_size // 2), F32),
                pltpu.VMEM((2, 5, tokens, hidden_size // 2), F32),
                dma((CORES, chips)), dma((2, 2)), dma((2,)), dma((2, 5)), dma((2, 5)),
            ],
            compiler_params=pltpu.CompilerParams(collective_id=1, has_side_effects=True, vmem_limit_bytes=VMEM_LIMIT),
            name='combine_scatter',
        )(expert_out, peer_out, heads, sides, hidden, shared_out)

    token_spec = P(('dp', 'ep'), None)
    expert_spec = P('ep', None, None)
    return jax.shard_map(
        local_step,
        mesh=mesh,
        in_specs=(token_spec, P(None), P(None, None), token_spec, expert_spec, expert_spec, expert_spec,
                  P(None, None), P(None, None), P(None, None)),
        out_specs=token_spec,
        check_vma=False,
    )
```

```python
import functools

import jax
import jax.numpy as jnp
from jax import lax
from jax.experimental import pallas as pl
from jax.experimental.pallas import tpu as pltpu
from jax.sharding import PartitionSpec as P

NORM_EPS = 1e-6
CORES = 2
VMEM_LIMIT = 67043328
F32 = jnp.float32
BF16 = jnp.bfloat16


def slots_of(side, first_expert, local_count, before):
    ids, weights = side[0:8], side[8:16]
    chosen, picked = [], []
    for e in range(8):
        hit = ids == (first_expert + e).astype(F32)
        chosen.append(jnp.sum(jnp.where(hit, 1.0, 0.0), axis=0, keepdims=True))
        picked.append(jnp.sum(jnp.where(hit, weights, 0.0), axis=0, keepdims=True))
    chosen = jnp.concatenate(chosen, axis=0)
    rank = jnp.dot(chosen.astype(BF16), before, preferred_element_type=F32)
    slot = jnp.where(chosen > 0.5, rank, -1000.0)
    return [slot[e:e + 1] for e in range(local_count)], picked[:local_count]


def place_of(group_size):
    chips = group_size // CORES
    me = lax.axis_index('ep')
    chip, core = me // CORES, me % CORES
    right = (chip + 1) % chips * CORES + core
    left = (chip + chips - 1) % chips * CORES + core
    return me, chip, core, right, left, chip * CORES + (1 - core)


def announce(neighbours):
    for device in neighbours:
        pl.semaphore_signal(pltpu.get_barrier_semaphore(), inc=1, device_id={'ep': device},
                            device_id_type=pl.DeviceIdType.MESH)


def meet(neighbours):
    pl.semaphore_wait(pltpu.get_barrier_semaphore(), len(neighbours))


def fill_before(before):
    row = lax.broadcasted_iota(jnp.int32, before.shape, 0)
    col = lax.broadcasted_iota(jnp.int32, before.shape, 1)
    before[...] = jnp.where(row < col, 1.0, 0.0).astype(BF16)


def remote(src, dst, send_sem, recv_sem, device):
    return pltpu.make_async_remote_copy(src_ref=src, dst_ref=dst, send_sem=send_sem, recv_sem=recv_sem,
                                        device_id={'ep': device}, device_id_type=pl.DeviceIdType.MESH)


def gather_kernel(group_size, capacity, slots, hidden_hbm, gain_hbm, router_hbm, idx_hbm,
                  sgate, sup, sdown, wgate, wup, wdown,
                  out_hbm, peer_hbm, head_hbm, side_hbm, shared_hbm,
                  gain_ref, router_ref, idx_ref, shared_ref, before_ref, rows, sides, x_ref, pick, gate_buf, up_buf, down_buf,
                  ring_s, ring_r, part_s, part_r, tring_s, tring_r, tpart_s, tpart_r, own_s, own_r,
                  head_s, head_r, peer_s, peer_r, load_sem, w_sem, out_sem):
    me, _, core, right, left, partner = place_of(group_size)
    local_count, hidden_size, ff = wgate.shape
    tokens = hidden_hbm.shape[0]
    half = tokens // 2
    half_cols = hidden_size // 2
    last = group_size // CORES - 1
    mine = pl.multiple_of(core * tokens, tokens)
    other = pl.multiple_of((1 - core) * tokens, tokens)

    def order(way, n):
        return min(2 * n + 1 + way, last)

    def piece(way, i, base):
        r = i % 2 if way == 0 else 1 - i % 2
        return rows.at[order(way, i // 2), pl.ds(pl.multiple_of(base + r * half, half), half)]

    def ring(way, i):
        n = i // 2
        r = i % 2 if way == 0 else 1 - i % 2
        src = 0 if n == 0 else order(way, n - 1)
        return remote(rows.at[src, pl.ds(pl.multiple_of(mine + r * half, half), half)], piece(way, i, mine),
                      ring_s.at[way, i], ring_r.at[way, i], right if way == 0 else left)

    def part(way, i, base):
        return remote(piece(way, i, base), piece(way, i, base), part_s.at[way, i], part_r.at[way, i], partner)

    def tring(way, n):
        src = 0 if n == 0 else 2 * (n - 1) + 1 + way
        return remote(sides.at[src, core], sides.at[2 * n + 1 + way, core],
                      tring_s.at[way, n], tring_r.at[way, n], right if way == 0 else left)

    def tpart(way, n, who):
        place = sides.at[2 * n + 1 + way, who]
        return remote(place, place, tpart_s.at[way, n], tpart_r.at[way, n], partner)

    def own_part(base):
        place = rows.at[0, pl.ds(base, tokens)]
        return remote(place, place, own_s.at[0], own_r.at[0], partner)

    def own_tpart(who):
        place = sides.at[0, who]
        return remote(place, place, own_s.at[1], own_r.at[1], partner)

    sends = 7

    def send(i):
        for way in range(2):
            ring(way, i).start()
            if i % 2 == 0 and i > 0:
                tring(way, i // 2).start()

    def service(i):
        for way in range(2):
            ring(way, i).wait_recv()
            if i % 2 == 0:
                tring(way, i // 2).wait_recv()
        if i + 2 < sends:
            send(i + 2)
        for way in range(2):
            part(way, i, mine).start()
            if i % 2 == 0:
                tpart(way, i // 2, core).start()

    def partner_arrived(i):
        for way in range(2):
            part(way, i, other).wait_recv()
            if i % 2 == 0:
                tpart(way, i // 2, 1 - core).wait_recv()

    beside = (right - core, left - core)

    def head(way, step, e, cc, source):
        chip_row, cols = (((2, 0), (1, 1)), ((2, 1), (0, 0)))[way][step]
        return remote(x_ref.at[e, chip_row, pl.ds(cc * HEAD_START, HEAD_ROWS), cols * half_cols:(cols + 1) * half_cols],
                      head_hbm.at[way, step, source, e], head_s.at[way, step, e, cc], head_r.at[way, step, e, source],
                      beside[way] + cc)

    def send_heads(step, e):
        for way in range(2):
            for cc in range(CORES):
                head(way, step, e, cc, core).start()

    def peer(turn, first, count, e):
        return remote(x_ref.at[e, 0:count], peer_hbm.at[e, pl.ds(first, count)], peer_s.at[turn, e], peer_r.at[turn, e], partner)

    loads = (pltpu.make_async_copy(hidden_hbm, rows.at[0, pl.ds(mine, tokens)], load_sem.at[0]),
             pltpu.make_async_copy(gain_hbm, gain_ref, load_sem.at[1]),
             pltpu.make_async_copy(router_hbm, router_ref, load_sem.at[2]),
             pltpu.make_async_copy(idx_hbm, idx_ref, load_sem.at[3]))
    for copy in loads:
        copy.start()
    store_shared = pltpu.make_async_copy(shared_ref, shared_hbm, load_sem.at[4])
    store_side = pltpu.make_async_copy(sides.at[0:group_size // CORES], side_hbm, load_sem.at[5])

    def normalise():
        block = 32

        def one(i, carry):
            place = pl.ds(pl.multiple_of(mine + i * block, block), block)
            x = rows[0, place, :].astype(F32)
            inv_rms = lax.rsqrt(jnp.mean(x * x, axis=-1, keepdims=True) + NORM_EPS)
            rows[0, place, :] = (x * inv_rms * gain_ref[...]).astype(BF16)
            return carry
        lax.fori_loop(0, tokens // block, one, 0)

    def route():
        x = rows[0, pl.ds(mine, tokens), :]
        logits = lax.dot_general(router_ref[...], x, (((1,), (1,)), ((), ())), preferred_element_type=F32)
        top = jnp.exp(logits - jnp.max(logits, axis=0, keepdims=True))
        probs = top / jnp.sum(top, axis=0, keepdims=True)
        experts_id = lax.broadcasted_iota(jnp.int32, probs.shape, 0)
        sides[0, core] = jnp.full((16, tokens), -1.0, F32)
        for j in range(idx_ref.shape[0]):
            idx = idx_ref[j:j + 1, :]
            sides[0, core, j:j + 1, :] = idx.astype(F32)
            sides[0, core, 8 + j:9 + j, :] = jnp.sum(jnp.where(experts_id == idx, probs, 0.0), axis=0, keepdims=True)

    def gate_copies(slot, gate, up):
        return (pltpu.make_async_copy(gate, gate_buf.at[slot], w_sem.at[slot]),
                pltpu.make_async_copy(up, up_buf.at[slot], w_sem.at[2 + slot]))

    def start_gate(slot, gate, up):
        for copy in gate_copies(slot, gate, up):
            copy.start()

    def down_copy(slot, down):
        return pltpu.make_async_copy(down, down_buf.at[slot], w_sem.at[4 + slot])

    def shared_cols(ref, i):
        return ref.at[:, pl.ds(pl.multiple_of(i * ff, 128), ff)]

    neighbours = [device + cc for device in beside for cc in range(CORES)] + [partner]
    announce(neighbours)
    start_gate(0, shared_cols(sgate, 0), shared_cols(sup, 0))
    down_copy(0, sdown.at[0:ff]).start()
    start_gate(1, shared_cols(sgate, 1), shared_cols(sup, 1))
    down_copy(1, sdown.at[ff:2 * ff]).start()
    fill_before(before_ref)
    for copy in loads:
        copy.wait()
    normalise()
    meet(neighbours)
    send(0)
    send(1)
    own_part(mine).start()
    route()
    for way in range(2):
        tring(way, 0).start()
    own_tpart(core).start()

    def swiglu(x, slot, fresh, next_gate, next_down):
        if fresh:
            for copy in gate_copies(slot, wgate.at[0], wup.at[0]):
                copy.wait()
        gate_out = jnp.dot(x, gate_buf[slot], preferred_element_type=F32)
        up_out = jnp.dot(x, up_buf[slot], preferred_element_type=F32)
        act = (jax.nn.silu(gate_out) * up_out).astype(BF16)
        next_gate()
        if fresh:
            down_copy(slot, wdown.at[0]).wait()
        out = jnp.dot(act, down_buf[slot], preferred_element_type=F32)
        next_down()
        return out

    def nothing():
        pass

    shared_parts = 2

    def shared(i, carry):
        slot = i % 2

        shared_ref[...] += swiglu(rows[0, pl.ds(mine, tokens), :], slot, True,
                                  lambda: start_gate(slot, wgate.at[i], wup.at[i]), lambda: down_copy(slot, wdown.at[i]).start())
        return carry

    shared_ref[...] = jnp.zeros_like(shared_ref)
    lax.fori_loop(0, shared_parts, shared, 0)

    def dispatch(base, start, count):
        def one(ch, carry):
            for cc in range(CORES):
                slot, _ = slots_of(sides[ch, cc], me * local_count, local_count, before_ref[...])
                row_id = lax.broadcasted_iota(jnp.int32, (slots, tokens), 0).astype(F32)
                for e in range(local_count):
                    hit = row_id == slot[e] + float(capacity * cc)
                    pick[e * slots:(e + 1) * slots, cc * tokens:(cc + 1) * tokens] = jnp.where(hit, 1.0, 0.0).astype(BF16)
            step = min(512, hidden_size)
            for n in range(0, hidden_size, step):
                got = jnp.dot(pick[...], rows[ch, :, n:n + step], preferred_element_type=F32).astype(BF16)
                for e in range(local_count):
                    x_ref[e, ch - base, :, n:n + step] = got[e * slots:(e + 1) * slots]
            return carry
        lax.fori_loop(start, start + count, one, 0)

    def stage_copy(e, first, count):
        return pltpu.make_async_copy(x_ref.at[e, 0:count], out_hbm.at[e, pl.ds(first, count)], out_sem.at[e])

    def mlp(e, slot, begin, count, fresh, next_gate, next_down):
        x = x_ref[e, begin:begin + count].reshape(count * slots, hidden_size)
        out = swiglu(x, slot, fresh, next_gate, next_down).astype(BF16)
        x_ref[e, begin:begin + count] = out.reshape(count, slots, hidden_size)

    def gate_after(e, slot):
        ahead = (e + 2) % local_count
        start_gate(slot, wgate.at[ahead], wup.at[ahead])

    def down_after(e, slot):
        down_copy(slot, wdown.at[(e + 2) % local_count]).start()

    def put(turn, first, count, e):
        stage_copy(e, first, count).start()
        peer(turn, first, count, e).start()

    def experts(turn, first, count, middle):
        def one(e, carry):
            @pl.when(e == local_count // 2)
            def _():
                service(middle)
            mlp(e, e % 2, 0, count, True, lambda: gate_after(e, e % 2), lambda: down_after(e, e % 2))
            put(turn, first, count, e)
            return carry
        lax.fori_loop(0, local_count, one, 0)

    def last_experts(turn, first, count):
        def near(e, carry):
            mlp(e, e % 2, 0, count - 1, True, nothing, nothing)
            send_heads(1, e)
            return carry

        def far(e, carry):
            mlp(e, e % 2, count - 1, 1, False, lambda: gate_after(e, e % 2), lambda: down_after(e, e % 2))
            send_heads(0, e)
            put(turn, first, count, e)
            return carry

        def both(e, carry):
            mlp(e, e % 2, 0, count, True, nothing, nothing)
            send_heads(1, e)
            send_heads(0, e)
            put(turn, first, count, e)
            return carry

        lax.fori_loop(0, 2, near, 0)
        service(6)
        partner_arrived(6)
        dispatch(first, first + count - 1, 1)
        lax.fori_loop(0, 2, far, 0)
        lax.fori_loop(2, local_count, both, 0)

    def finish(turn, first, count):
        for e in range(local_count):
            stage_copy(e, first, count).wait()
            peer(turn, first, count, e).wait_send()

    service(0)
    own_part(other).wait_recv()
    own_tpart(1 - core).wait_recv()
    dispatch(0, 0, 1)
    store_shared.start()
    service(1)
    partner_arrived(0)
    partner_arrived(1)
    dispatch(0, 1, 2)
    experts(0, 0, 3, 2)
    finish(0, 0, 3)
    service(3)
    partner_arrived(2)
    partner_arrived(3)
    dispatch(3, 3, 2)
    experts(1, 3, 2, 4)
    finish(1, 3, 2)
    service(5)
    partner_arrived(4)
    partner_arrived(5)
    dispatch(5, 5, 2)
    last_experts(2, 5, 3)
    finish(2, 5, 3)
    store_side.start()
    for way in range(2):
        for i in range(sends):
            ring(way, i).wait_send()
            part(way, i, mine).wait_send()
            if i % 2 == 0:
                tring(way, i // 2).wait_send()
                tpart(way, i // 2, core).wait_send()
    own_part(mine).wait_send()
    own_tpart(core).wait_send()
    for turn, (first, count) in enumerate(((0, 3), (3, 2), (5, 3))):
        for e in range(local_count):
            peer(turn, first, count, e).wait_recv()
    store_shared.wait()
    store_side.wait()

    def settle(e, carry):
        for step in range(2):
            for way in range(2):
                for cc in range(CORES):
                    head(way, step, e, cc, cc).wait_recv()
                    head(way, step, e, cc, cc).wait_send()
        return carry
    lax.fori_loop(0, local_count, settle, 0)


def scatter_kernel(group_size, capacity, rows_hbm, peer_hbm, head_hbm, side_hbm, hidden_hbm, shared_hbm, out_ref,
                   side_ref, before_ref, hidden_ref, shared_ref, rows, heads, acc, ring_in, load_sem, head_sem, base_sem, ring_s, ring_r):
    _, chip, core, right, left, _ = place_of(group_size)
    _, local_count, chips, _, hidden_size = rows.shape
    tokens = hidden_ref.shape[0]
    half = hidden_size // 2
    last = chips - 1
    steps = 5
    window = pl.ds(pl.multiple_of(core * HEAD_START, HEAD_START), WINDOW)

    def load(ch):
        return (pltpu.make_async_copy(rows_hbm.at[:, ch, window], rows.at[core, :, ch], load_sem.at[0, ch]),
                pltpu.make_async_copy(peer_hbm.at[:, ch, window], rows.at[1 - core, :, ch], load_sem.at[1, ch]))

    def load_head(way, i):
        return pltpu.make_async_copy(head_hbm.at[way, i], heads.at[way, i, :, :, 0:HEAD_ROWS], head_sem.at[way, i])

    neighbours = (right, left)
    announce(neighbours)
    load_side = pltpu.make_async_copy(side_hbm, side_ref, base_sem.at[2])
    load_side.start()
    for i in range(2):
        for way in range(2):
            load_head(way, i).start()
            for copy in load((last - 1, last - 2, 4, 3)[2 * i + way]):
                copy.start()
    for ch in (2, 1, 0):
        for copy in load(ch):
            copy.start()
    load_base = (pltpu.make_async_copy(hidden_hbm, hidden_ref, base_sem.at[0]),
                 pltpu.make_async_copy(shared_hbm, shared_ref, base_sem.at[1]))
    for copy in load_base:
        copy.start()
    fill_before(before_ref)
    heads[:, :, :, :, HEAD_ROWS:WINDOW, :] = jnp.zeros((2, 2, CORES, local_count, WINDOW - HEAD_ROWS, half), BF16)

    def ring(way, i):
        return remote(acc.at[way, i % 2], ring_in.at[way, i], ring_s.at[way, i], ring_r.at[way, i],
                      right if way == 0 else left)

    def mix_of(ch, from_chip):
        count = CORES * local_count
        slot, weight = slots_of(side_ref[ch, core], from_chip * count, count, before_ref[...])
        row_id = lax.broadcasted_iota(jnp.int32, (WINDOW, tokens), 0).astype(F32)
        shift = (core * (capacity - HEAD_START)).astype(F32)
        return [jnp.where(row_id == slot[e] + shift, weight[e], 0.0) for e in range(count)]

    def unit(ch, h, way, i):
        col = pl.multiple_of(h * half, half)
        mix = mix_of(ch, chip)
        picked = [rows[cc, e, ch, :, pl.ds(col, half)] for cc in range(CORES) for e in range(local_count)]
        if i < 2:
            mix += mix_of(ch, (left + way * (right - left)) // CORES)
            picked += [heads[way, i, cc, e] for cc in range(CORES) for e in range(local_count)]
        mix = jnp.concatenate(mix, axis=0)
        picked = jnp.concatenate(picked, axis=0)
        high = mix.astype(BF16)
        rest = mix - high.astype(F32)
        mid = rest.astype(BF16)
        low = (rest - mid.astype(F32)).astype(BF16)
        total = jnp.dot(high.T, picked, preferred_element_type=F32)
        total += jnp.dot(mid.T, picked, preferred_element_type=F32)
        return total + jnp.dot(low.T, picked, preferred_element_type=F32)

    def units(i, chans, halves):
        def one(way, carry):
            ch = chans[0] + way * (chans[1] - chans[0])
            h = halves[0] + way * (halves[1] - halves[0])
            acc[way, i % 2] = unit(ch, h, way, i)
            return carry
        lax.fori_loop(0, 2, one, 0)

    load_side.wait()
    loaded = set()

    def ensure(ch):
        if ch not in loaded:
            loaded.add(ch)
            for copy in load(ch):
                copy.wait()

    for i in range(steps):
        k = 3 - (i + 1) // 2
        chans = (2 * k, 2 * k - 1)
        for ch in chans:
            ensure(ch)
        for way in range(2):
            if i < 2:
                load_head(way, i).wait()
            else:
                ring(way, i - 2).wait_send()
        units(i, chans, (i % 2, 1 - i % 2))
        if i == 0:
            meet(neighbours)
        for way in range(2):
            if i >= 2:
                ring(way, i - 2).wait_recv()
                acc[way, i % 2] = acc[way, i % 2] + ring_in[way, i - 2]
            ring(way, i).start()
    ensure(0)
    for way in range(2):
        ring(way, steps - 2).wait_send()
    units(steps, (0, 0), (0, 1))
    for copy in load_base:
        copy.wait()
    for h in range(2):
        ring(1 - h, steps - 2).wait_recv()
        cols = slice(h * half, (h + 1) * half)
        acc[h, steps % 2] = (acc[h, steps % 2] + ring_in[1 - h, steps - 2]
                             + shared_ref[:, cols] + hidden_ref[:, cols].astype(F32))
    for h in range(2):
        ring(h, steps - 1).wait_recv()
        cols = slice(h * half, (h + 1) * half)
        out_ref[:, cols] = (acc[h, steps % 2] + ring_in[h, steps - 1]).astype(BF16)
    for way in range(2):
        ring(way, steps - 1).wait_send()


WINDOW = 48
HEAD_START = 32
HEAD_ROWS = 40


def solution(mesh):
    group_size = mesh.shape['ep']
    chips = group_size // CORES

    def local_step(hidden, norm_gain, router_w, topk_idx, w_gate, w_up, w_down, shared_gate, shared_up, shared_down):
        tokens, hidden_size = hidden.shape
        num_experts = router_w.shape[1]
        local_count, _, ff = w_gate.shape
        capacity = 3 * tokens * topk_idx.shape[1] // (2 * num_experts)
        slots = (CORES * capacity + 15) // 16 * 16
        hbm = pl.BlockSpec(memory_space=pl.ANY)
        vmem = pl.BlockSpec(memory_space=pltpu.VMEM)
        dma = pltpu.SemaphoreType.DMA
        expert_out, peer_out, heads, sides, shared_out = pl.pallas_call(
            functools.partial(gather_kernel, group_size, capacity, slots),
            in_specs=[hbm] * 10,
            out_specs=(hbm,) * 5,
            out_shape=(jax.ShapeDtypeStruct((local_count, chips, slots, hidden_size), BF16),
                       jax.ShapeDtypeStruct((local_count, chips, slots, hidden_size), BF16),
                       jax.ShapeDtypeStruct((2, 2, CORES, local_count, HEAD_ROWS, hidden_size // 2), BF16),
                       jax.ShapeDtypeStruct((chips, CORES, 16, tokens), F32),
                       jax.ShapeDtypeStruct((tokens, hidden_size), F32)),
            scratch_shapes=[
                pltpu.VMEM((1, hidden_size), F32),
                pltpu.VMEM((num_experts, hidden_size), BF16),
                pltpu.VMEM((topk_idx.shape[1], tokens), jnp.int32),
                pltpu.VMEM((tokens, hidden_size), F32),
                pltpu.VMEM((tokens, tokens), BF16),
                pltpu.VMEM((chips, CORES * tokens, hidden_size), BF16),
                pltpu.VMEM((chips + 1, CORES, 16, tokens), F32),
                pltpu.VMEM((local_count, 3, slots, hidden_size), BF16),
                pltpu.VMEM((local_count * slots, CORES * tokens), BF16),
                pltpu.VMEM((2, hidden_size, ff), BF16),
                pltpu.VMEM((2, hidden_size, ff), BF16),
                pltpu.VMEM((2, ff, hidden_size), BF16),
                dma((2, 7)), dma((2, 7)), dma((2, 7)), dma((2, 7)),
                dma((2, 4)), dma((2, 4)), dma((2, 4)), dma((2, 4)),
                dma((2,)), dma((2,)), dma((2, 2, local_count, CORES)), dma((2, 2, local_count, CORES)),
                dma((3, local_count)), dma((3, local_count)),
                dma((6,)), dma((6,)), dma((local_count,)),
            ],
            compiler_params=pltpu.CompilerParams(collective_id=0, has_side_effects=True, vmem_limit_bytes=VMEM_LIMIT),
            name='gather_experts',
        )(hidden, norm_gain[None, :], router_w.T, topk_idx.T, shared_gate, shared_up, shared_down, w_gate, w_up, w_down)
        return pl.pallas_call(
            functools.partial(scatter_kernel, group_size, capacity),
            in_specs=[hbm] * 6,
            out_specs=vmem,
            out_shape=jax.ShapeDtypeStruct((tokens, hidden_size), BF16),
            scratch_shapes=[
                pltpu.VMEM((chips, CORES, 16, tokens), F32),
                pltpu.VMEM((tokens, tokens), BF16),
                pltpu.VMEM((tokens, hidden_size), BF16),
                pltpu.VMEM((tokens, hidden_size), F32),
                pltpu.VMEM((CORES, local_count, chips, WINDOW, hidden_size), BF16),
                pltpu.VMEM((2, 2, CORES, local_count, WINDOW, hidden_size // 2), BF16),
                pltpu.VMEM((2, 2, tokens, hidden_size // 2), F32),
                pltpu.VMEM((2, 5, tokens, hidden_size // 2), F32),
                dma((CORES, chips)), dma((2, 2)), dma((3,)), dma((2, 5)), dma((2, 5)),
            ],
            compiler_params=pltpu.CompilerParams(collective_id=1, has_side_effects=True, vmem_limit_bytes=VMEM_LIMIT),
            name='combine_scatter',
        )(expert_out, peer_out, heads, sides, hidden, shared_out)

    token_spec = P(('dp', 'ep'), None)
    expert_spec = P('ep', None, None)
    return jax.shard_map(
        local_step,
        mesh=mesh,
        in_specs=(token_spec, P(None), P(None, None), token_spec, expert_spec, expert_spec, expert_spec,
                  P(None, None), P(None, None), P(None, None)),
        out_specs=token_spec,
        check_vma=False,
    )
```

```python
import functools

import jax
import jax.numpy as jnp
from jax import lax
from jax.experimental import pallas as pl
from jax.experimental.pallas import tpu as pltpu
from jax.sharding import PartitionSpec as P

NORM_EPS = 1e-6
CORES = 2
VMEM_LIMIT = 67043328
F32 = jnp.float32
BF16 = jnp.bfloat16


def slots_of(side, first_expert, local_count, before):
    ids, weights = side[0:8], side[8:16]
    chosen, picked = [], []
    for e in range(8):
        hit = ids == (first_expert + e).astype(F32)
        chosen.append(jnp.sum(jnp.where(hit, 1.0, 0.0), axis=0, keepdims=True))
        picked.append(jnp.sum(jnp.where(hit, weights, 0.0), axis=0, keepdims=True))
    chosen = jnp.concatenate(chosen, axis=0)
    rank = jnp.dot(chosen.astype(BF16), before, preferred_element_type=F32)
    slot = jnp.where(chosen > 0.5, rank, -1000.0)
    return [slot[e:e + 1] for e in range(local_count)], picked[:local_count]


def place_of(group_size):
    chips = group_size // CORES
    me = lax.axis_index('ep')
    chip, core = me // CORES, me % CORES
    right = (chip + 1) % chips * CORES + core
    left = (chip + chips - 1) % chips * CORES + core
    return me, chip, core, right, left, chip * CORES + (1 - core)


def announce(neighbours):
    for device in neighbours:
        pl.semaphore_signal(pltpu.get_barrier_semaphore(), inc=1, device_id={'ep': device},
                            device_id_type=pl.DeviceIdType.MESH)


def meet(neighbours):
    pl.semaphore_wait(pltpu.get_barrier_semaphore(), len(neighbours))


def fill_before(before):
    row = lax.broadcasted_iota(jnp.int32, before.shape, 0)
    col = lax.broadcasted_iota(jnp.int32, before.shape, 1)
    before[...] = jnp.where(row < col, 1.0, 0.0).astype(BF16)


def remote(src, dst, send_sem, recv_sem, device):
    return pltpu.make_async_remote_copy(src_ref=src, dst_ref=dst, send_sem=send_sem, recv_sem=recv_sem,
                                        device_id={'ep': device}, device_id_type=pl.DeviceIdType.MESH)


def gather_kernel(group_size, capacity, slots, hidden_hbm, gain_hbm, router_hbm, idx_hbm,
                  sgate, sup, sdown, wgate, wup, wdown,
                  out_hbm, peer_hbm, head_hbm, side_hbm, shared_hbm,
                  gain_ref, router_ref, idx_ref, shared_ref, before_ref, rows, sides, x_ref, pick, gate_buf, up_buf, down_buf,
                  ring_s, ring_r, part_s, part_r, tring_s, tring_r, tpart_s, tpart_r, own_s, own_r,
                  head_s, head_r, peer_s, peer_r, load_sem, w_sem, out_sem):
    me, _, core, right, left, partner = place_of(group_size)
    local_count, hidden_size, ff = wgate.shape
    tokens = hidden_hbm.shape[0]
    half = tokens // 2
    half_cols = hidden_size // 2
    last = group_size // CORES - 1
    mine = pl.multiple_of(core * tokens, tokens)
    other = pl.multiple_of((1 - core) * tokens, tokens)

    def order(way, n):
        return min(2 * n + 1 + way, last)

    def piece(way, i, base):
        r = i % 2 if way == 0 else 1 - i % 2
        return rows.at[order(way, i // 2), pl.ds(pl.multiple_of(base + r * half, half), half)]

    def ring(way, i):
        n = i // 2
        r = i % 2 if way == 0 else 1 - i % 2
        src = 0 if n == 0 else order(way, n - 1)
        return remote(rows.at[src, pl.ds(pl.multiple_of(mine + r * half, half), half)], piece(way, i, mine),
                      ring_s.at[way, i], ring_r.at[way, i], right if way == 0 else left)

    def part(way, i, base):
        return remote(piece(way, i, base), piece(way, i, base), part_s.at[way, i], part_r.at[way, i], partner)

    def tring(way, n):
        src = 0 if n == 0 else 2 * (n - 1) + 1 + way
        return remote(sides.at[src, core], sides.at[2 * n + 1 + way, core],
                      tring_s.at[way, n], tring_r.at[way, n], right if way == 0 else left)

    def tpart(way, n, who):
        place = sides.at[2 * n + 1 + way, who]
        return remote(place, place, tpart_s.at[way, n], tpart_r.at[way, n], partner)

    def own_part(base):
        place = rows.at[0, pl.ds(base, tokens)]
        return remote(place, place, own_s.at[0], own_r.at[0], partner)

    def own_tpart(who):
        place = sides.at[0, who]
        return remote(place, place, own_s.at[1], own_r.at[1], partner)

    sends = 7

    def send(i):
        for way in range(2):
            ring(way, i).start()
            if i % 2 == 0 and i > 0:
                tring(way, i // 2).start()

    def service(i):
        for way in range(2):
            ring(way, i).wait_recv()
            if i % 2 == 0:
                tring(way, i // 2).wait_recv()
        if i + 2 < sends:
            send(i + 2)
        for way in range(2):
            part(way, i, mine).start()
            if i % 2 == 0:
                tpart(way, i // 2, core).start()

    def partner_arrived(i):
        for way in range(2):
            part(way, i, other).wait_recv()
            if i % 2 == 0:
                tpart(way, i // 2, 1 - core).wait_recv()

    beside = (right - core, left - core)

    def head(way, step, e, cc, source):
        chip_row, cols = (((2, 0), (1, 1)), ((2, 1), (0, 0)))[way][step]
        return remote(x_ref.at[e, chip_row, pl.ds(cc * HEAD_START, HEAD_ROWS), cols * half_cols:(cols + 1) * half_cols],
                      head_hbm.at[way, step, source, e], head_s.at[way, step, e, cc], head_r.at[way, step, e, source],
                      beside[way] + cc)

    def send_heads(step, e):
        for way in range(2):
            for cc in range(CORES):
                head(way, step, e, cc, core).start()

    def peer(turn, first, count, e):
        return remote(x_ref.at[e, 0:count], peer_hbm.at[e, pl.ds(first, count)], peer_s.at[turn, e], peer_r.at[turn, e], partner)

    loads = (pltpu.make_async_copy(hidden_hbm, rows.at[0, pl.ds(mine, tokens)], load_sem.at[0]),
             pltpu.make_async_copy(gain_hbm, gain_ref, load_sem.at[1]),
             pltpu.make_async_copy(router_hbm, router_ref, load_sem.at[2]),
             pltpu.make_async_copy(idx_hbm, idx_ref, load_sem.at[3]))
    for copy in loads:
        copy.start()
    store_shared = pltpu.make_async_copy(shared_ref, shared_hbm, load_sem.at[4])
    store_side = pltpu.make_async_copy(sides.at[0:group_size // CORES], side_hbm, load_sem.at[5])

    def normalise():
        block = 32

        def one(i, carry):
            place = pl.ds(pl.multiple_of(mine + i * block, block), block)
            x = rows[0, place, :].astype(F32)
            inv_rms = lax.rsqrt(jnp.mean(x * x, axis=-1, keepdims=True) + NORM_EPS)
            rows[0, place, :] = (x * inv_rms * gain_ref[...]).astype(BF16)
            return carry
        lax.fori_loop(0, tokens // block, one, 0)

    def route():
        x = rows[0, pl.ds(mine, tokens), :]
        logits = lax.dot_general(router_ref[...], x, (((1,), (1,)), ((), ())), preferred_element_type=F32)
        top = jnp.exp(logits - jnp.max(logits, axis=0, keepdims=True))
        probs = top / jnp.sum(top, axis=0, keepdims=True)
        experts_id = lax.broadcasted_iota(jnp.int32, probs.shape, 0)
        sides[0, core] = jnp.full((16, tokens), -1.0, F32)
        for j in range(idx_ref.shape[0]):
            idx = idx_ref[j:j + 1, :]
            sides[0, core, j:j + 1, :] = idx.astype(F32)
            sides[0, core, 8 + j:9 + j, :] = jnp.sum(jnp.where(experts_id == idx, probs, 0.0), axis=0, keepdims=True)

    def gate_copies(slot, gate, up):
        return (pltpu.make_async_copy(gate, gate_buf.at[slot], w_sem.at[slot]),
                pltpu.make_async_copy(up, up_buf.at[slot], w_sem.at[2 + slot]))

    def start_gate(slot, gate, up):
        for copy in gate_copies(slot, gate, up):
            copy.start()

    def down_copy(slot, down):
        return pltpu.make_async_copy(down, down_buf.at[slot], w_sem.at[4 + slot])

    def shared_cols(ref, i):
        return ref.at[:, pl.ds(pl.multiple_of(i * ff, 128), ff)]

    neighbours = [device + cc for device in beside for cc in range(CORES)] + [partner]
    announce(neighbours)
    fill_before(before_ref)
    for copy in loads:
        copy.wait()
    start_gate(0, shared_cols(sgate, 0), shared_cols(sup, 0))
    down_copy(0, sdown.at[0:ff]).start()
    start_gate(1, shared_cols(sgate, 1), shared_cols(sup, 1))
    down_copy(1, sdown.at[ff:2 * ff]).start()
    normalise()
    meet(neighbours)
    send(0)
    send(1)
    own_part(mine).start()
    route()
    for way in range(2):
        tring(way, 0).start()
    own_tpart(core).start()

    def swiglu(x, slot, fresh, next_gate, next_down):
        if fresh:
            for copy in gate_copies(slot, wgate.at[0], wup.at[0]):
                copy.wait()
        gate_out = jnp.dot(x, gate_buf[slot], preferred_element_type=F32)
        up_out = jnp.dot(x, up_buf[slot], preferred_element_type=F32)
        act = (jax.nn.silu(gate_out) * up_out).astype(BF16)
        next_gate()
        if fresh:
            down_copy(slot, wdown.at[0]).wait()
        out = jnp.dot(act, down_buf[slot], preferred_element_type=F32)
        next_down()
        return out

    def nothing():
        pass

    shared_parts = 2

    def shared(i, carry):
        slot = i % 2

        shared_ref[...] += swiglu(rows[0, pl.ds(mine, tokens), :], slot, True,
                                  lambda: start_gate(slot, wgate.at[i], wup.at[i]), lambda: down_copy(slot, wdown.at[i]).start())
        return carry

    shared_ref[...] = jnp.zeros_like(shared_ref)
    lax.fori_loop(0, shared_parts, shared, 0)

    def dispatch(base, start, count):
        def one(ch, carry):
            for cc in range(CORES):
                slot, _ = slots_of(sides[ch, cc], me * local_count, local_count, before_ref[...])
                row_id = lax.broadcasted_iota(jnp.int32, (slots, tokens), 0).astype(F32)
                for e in range(local_count):
                    hit = row_id == slot[e] + float(capacity * cc)
                    pick[e * slots:(e + 1) * slots, cc * tokens:(cc + 1) * tokens] = jnp.where(hit, 1.0, 0.0).astype(BF16)
            step = min(512, hidden_size)
            for n in range(0, hidden_size, step):
                got = jnp.dot(pick[...], rows[ch, :, n:n + step], preferred_element_type=F32).astype(BF16)
                for e in range(local_count):
                    x_ref[e, ch - base, :, n:n + step] = got[e * slots:(e + 1) * slots]
            return carry
        lax.fori_loop(start, start + count, one, 0)

    def stage_copy(e, first, count):
        return pltpu.make_async_copy(x_ref.at[e, 0:count], out_hbm.at[e, pl.ds(first, count)], out_sem.at[e])

    def mlp(e, slot, begin, count, fresh, next_gate, next_down):
        x = x_ref[e, begin:begin + count].reshape(count * slots, hidden_size)
        out = swiglu(x, slot, fresh, next_gate, next_down).astype(BF16)
        x_ref[e, begin:begin + count] = out.reshape(count, slots, hidden_size)

    def gate_after(e, slot):
        ahead = (e + 2) % local_count
        start_gate(slot, wgate.at[ahead], wup.at[ahead])

    def down_after(e, slot):
        down_copy(slot, wdown.at[(e + 2) % local_count]).start()

    def put(turn, first, count, e):
        stage_copy(e, first, count).start()
        peer(turn, first, count, e).start()

    def experts(turn, first, count, middle):
        def one(e, carry):
            @pl.when(e == local_count // 2)
            def _():
                service(middle)
            mlp(e, e % 2, 0, count, True, lambda: gate_after(e, e % 2), lambda: down_after(e, e % 2))
            put(turn, first, count, e)
            return carry
        lax.fori_loop(0, local_count, one, 0)

    def last_experts(turn, first, count):
        def near(e, carry):
            mlp(e, e % 2, 0, count - 1, True, nothing, nothing)
            send_heads(1, e)
            return carry

        def far(e, carry):
            mlp(e, e % 2, count - 1, 1, False, lambda: gate_after(e, e % 2), lambda: down_after(e, e % 2))
            send_heads(0, e)
            put(turn, first, count, e)
            return carry

        def both(e, carry):
            mlp(e, e % 2, 0, count, True, nothing, nothing)
            send_heads(1, e)
            send_heads(0, e)
            put(turn, first, count, e)
            return carry

        lax.fori_loop(0, 2, near, 0)
        service(6)
        partner_arrived(6)
        dispatch(first, first + count - 1, 1)
        lax.fori_loop(0, 2, far, 0)
        lax.fori_loop(2, local_count, both, 0)

    def finish(turn, first, count):
        for e in range(local_count):
            stage_copy(e, first, count).wait()
            peer(turn, first, count, e).wait_send()

    service(0)
    own_part(other).wait_recv()
    own_tpart(1 - core).wait_recv()
    dispatch(0, 0, 1)
    store_shared.start()
    service(1)
    partner_arrived(0)
    partner_arrived(1)
    dispatch(0, 1, 2)
    experts(0, 0, 3, 2)
    finish(0, 0, 3)
    service(3)
    partner_arrived(2)
    partner_arrived(3)
    dispatch(3, 3, 2)
    experts(1, 3, 2, 4)
    finish(1, 3, 2)
    service(5)
    partner_arrived(4)
    partner_arrived(5)
    dispatch(5, 5, 2)
    last_experts(2, 5, 3)
    finish(2, 5, 3)
    store_side.start()
    for way in range(2):
        for i in range(sends):
            ring(way, i).wait_send()
            part(way, i, mine).wait_send()
            if i % 2 == 0:
                tring(way, i // 2).wait_send()
                tpart(way, i // 2, core).wait_send()
    own_part(mine).wait_send()
    own_tpart(core).wait_send()
    for turn, (first, count) in enumerate(((0, 3), (3, 2), (5, 3))):
        for e in range(local_count):
            peer(turn, first, count, e).wait_recv()
    store_shared.wait()
    store_side.wait()

    def settle(e, carry):
        for step in range(2):
            for way in range(2):
                for cc in range(CORES):
                    head(way, step, e, cc, cc).wait_recv()
                    head(way, step, e, cc, cc).wait_send()
        return carry
    lax.fori_loop(0, local_count, settle, 0)


def scatter_kernel(group_size, capacity, rows_hbm, peer_hbm, head_hbm, side_hbm, hidden_hbm, shared_hbm, out_ref,
                   side_ref, before_ref, hidden_ref, shared_ref, rows, heads, acc, ring_in, load_sem, head_sem, base_sem, ring_s, ring_r):
    _, chip, core, right, left, _ = place_of(group_size)
    _, local_count, chips, _, hidden_size = rows.shape
    tokens = hidden_ref.shape[0]
    half = hidden_size // 2
    last = chips - 1
    steps = 5
    window = pl.ds(pl.multiple_of(core * HEAD_START, HEAD_START), WINDOW)

    def load(ch):
        return (pltpu.make_async_copy(rows_hbm.at[:, ch, window], rows.at[core, :, ch], load_sem.at[0, ch]),
                pltpu.make_async_copy(peer_hbm.at[:, ch, window], rows.at[1 - core, :, ch], load_sem.at[1, ch]))

    def load_head(way, i):
        return pltpu.make_async_copy(head_hbm.at[way, i], heads.at[way, i, :, :, 0:HEAD_ROWS], head_sem.at[way, i])

    neighbours = (right, left)
    announce(neighbours)
    load_side = pltpu.make_async_copy(side_hbm, side_ref, base_sem.at[2])
    load_side.start()
    def start_loads(i):
        for way in range(2):
            load_head(way, i).start()
            for copy in load((last - 1, last - 2, 4, 3)[2 * i + way]):
                copy.start()

    load_base = (pltpu.make_async_copy(hidden_hbm, hidden_ref, base_sem.at[0]),
                 pltpu.make_async_copy(shared_hbm, shared_ref, base_sem.at[1]))
    start_loads(0)
    fill_before(before_ref)
    heads[:, :, :, :, HEAD_ROWS:WINDOW, :] = jnp.zeros((2, 2, CORES, local_count, WINDOW - HEAD_ROWS, half), BF16)

    def ring(way, i):
        return remote(acc.at[way, i % 2], ring_in.at[way, i], ring_s.at[way, i], ring_r.at[way, i],
                      right if way == 0 else left)

    def mix_of(ch, from_chip):
        count = CORES * local_count
        slot, weight = slots_of(side_ref[ch, core], from_chip * count, count, before_ref[...])
        row_id = lax.broadcasted_iota(jnp.int32, (WINDOW, tokens), 0).astype(F32)
        shift = (core * (capacity - HEAD_START)).astype(F32)
        return [jnp.where(row_id == slot[e] + shift, weight[e], 0.0) for e in range(count)]

    def unit(ch, h, way, i):
        col = pl.multiple_of(h * half, half)
        mix = mix_of(ch, chip)
        picked = [rows[cc, e, ch, :, pl.ds(col, half)] for cc in range(CORES) for e in range(local_count)]
        if i < 2:
            mix += mix_of(ch, (left + way * (right - left)) // CORES)
            picked += [heads[way, i, cc, e] for cc in range(CORES) for e in range(local_count)]
        mix = jnp.concatenate(mix, axis=0)
        picked = jnp.concatenate(picked, axis=0)
        high = mix.astype(BF16)
        rest = mix - high.astype(F32)
        mid = rest.astype(BF16)
        low = (rest - mid.astype(F32)).astype(BF16)
        total = jnp.dot(high.T, picked, preferred_element_type=F32)
        total += jnp.dot(mid.T, picked, preferred_element_type=F32)
        return total + jnp.dot(low.T, picked, preferred_element_type=F32)

    def units(i, chans, halves):
        def one(way, carry):
            ch = chans[0] + way * (chans[1] - chans[0])
            h = halves[0] + way * (halves[1] - halves[0])
            acc[way, i % 2] = unit(ch, h, way, i)
            return carry
        lax.fori_loop(0, 2, one, 0)

    load_side.wait()
    loaded = set()

    def ensure(ch):
        if ch not in loaded:
            loaded.add(ch)
            for copy in load(ch):
                copy.wait()

    for i in range(steps):
        k = 3 - (i + 1) // 2
        chans = (2 * k, 2 * k - 1)
        for ch in chans:
            ensure(ch)
        for way in range(2):
            if i < 2:
                load_head(way, i).wait()
            else:
                ring(way, i - 2).wait_send()
        if i == 0:
            start_loads(1)
            for ch in (2, 1, 0):
                for copy in load(ch):
                    copy.start()
            for copy in load_base:
                copy.start()
        units(i, chans, (i % 2, 1 - i % 2))
        if i == 0:
            meet(neighbours)
        for way in range(2):
            if i >= 2:
                ring(way, i - 2).wait_recv()
                acc[way, i % 2] = acc[way, i % 2] + ring_in[way, i - 2]
            ring(way, i).start()
    ensure(0)
    for way in range(2):
        ring(way, steps - 2).wait_send()
    units(steps, (0, 0), (0, 1))
    for copy in load_base:
        copy.wait()
    for h in range(2):
        ring(1 - h, steps - 2).wait_recv()
        cols = slice(h * half, (h + 1) * half)
        acc[h, steps % 2] = (acc[h, steps % 2] + ring_in[1 - h, steps - 2]
                             + shared_ref[:, cols] + hidden_ref[:, cols].astype(F32))
    for h in range(2):
        ring(h, steps - 1).wait_recv()
        cols = slice(h * half, (h + 1) * half)
        out_ref[:, cols] = (acc[h, steps % 2] + ring_in[h, steps - 1]).astype(BF16)
    for way in range(2):
        ring(way, steps - 1).wait_send()


WINDOW = 48
HEAD_START = 32
HEAD_ROWS = 40


def solution(mesh):
    group_size = mesh.shape['ep']
    chips = group_size // CORES

    def local_step(hidden, norm_gain, router_w, topk_idx, w_gate, w_up, w_down, shared_gate, shared_up, shared_down):
        tokens, hidden_size = hidden.shape
        num_experts = router_w.shape[1]
        local_count, _, ff = w_gate.shape
        capacity = 3 * tokens * topk_idx.shape[1] // (2 * num_experts)
        slots = (CORES * capacity + 15) // 16 * 16
        hbm = pl.BlockSpec(memory_space=pl.ANY)
        vmem = pl.BlockSpec(memory_space=pltpu.VMEM)
        dma = pltpu.SemaphoreType.DMA
        expert_out, peer_out, heads, sides, shared_out = pl.pallas_call(
            functools.partial(gather_kernel, group_size, capacity, slots),
            in_specs=[hbm] * 10,
            out_specs=(hbm,) * 5,
            out_shape=(jax.ShapeDtypeStruct((local_count, chips, slots, hidden_size), BF16),
                       jax.ShapeDtypeStruct((local_count, chips, slots, hidden_size), BF16),
                       jax.ShapeDtypeStruct((2, 2, CORES, local_count, HEAD_ROWS, hidden_size // 2), BF16),
                       jax.ShapeDtypeStruct((chips, CORES, 16, tokens), F32),
                       jax.ShapeDtypeStruct((tokens, hidden_size), F32)),
            scratch_shapes=[
                pltpu.VMEM((1, hidden_size), F32),
                pltpu.VMEM((num_experts, hidden_size), BF16),
                pltpu.VMEM((topk_idx.shape[1], tokens), jnp.int32),
                pltpu.VMEM((tokens, hidden_size), F32),
                pltpu.VMEM((tokens, tokens), BF16),
                pltpu.VMEM((chips, CORES * tokens, hidden_size), BF16),
                pltpu.VMEM((chips + 1, CORES, 16, tokens), F32),
                pltpu.VMEM((local_count, 3, slots, hidden_size), BF16),
                pltpu.VMEM((local_count * slots, CORES * tokens), BF16),
                pltpu.VMEM((2, hidden_size, ff), BF16),
                pltpu.VMEM((2, hidden_size, ff), BF16),
                pltpu.VMEM((2, ff, hidden_size), BF16),
                dma((2, 7)), dma((2, 7)), dma((2, 7)), dma((2, 7)),
                dma((2, 4)), dma((2, 4)), dma((2, 4)), dma((2, 4)),
                dma((2,)), dma((2,)), dma((2, 2, local_count, CORES)), dma((2, 2, local_count, CORES)),
                dma((3, local_count)), dma((3, local_count)),
                dma((6,)), dma((6,)), dma((local_count,)),
            ],
            compiler_params=pltpu.CompilerParams(collective_id=0, has_side_effects=True, vmem_limit_bytes=VMEM_LIMIT),
            name='gather_experts',
        )(hidden, norm_gain[None, :], router_w.T, topk_idx.T, shared_gate, shared_up, shared_down, w_gate, w_up, w_down)
        return pl.pallas_call(
            functools.partial(scatter_kernel, group_size, capacity),
            in_specs=[hbm] * 6,
            out_specs=vmem,
            out_shape=pltpu.VMEM((tokens, hidden_size), BF16),
            scratch_shapes=[
                pltpu.VMEM((chips, CORES, 16, tokens), F32),
                pltpu.VMEM((tokens, tokens), BF16),
                pltpu.VMEM((tokens, hidden_size), BF16),
                pltpu.VMEM((tokens, hidden_size), F32),
                pltpu.VMEM((CORES, local_count, chips, WINDOW, hidden_size), BF16),
                pltpu.VMEM((2, 2, CORES, local_count, WINDOW, hidden_size // 2), BF16),
                pltpu.VMEM((2, 2, tokens, hidden_size // 2), F32),
                pltpu.VMEM((2, 5, tokens, hidden_size // 2), F32),
                dma((CORES, chips)), dma((2, 2)), dma((3,)), dma((2, 5)), dma((2, 5)),
            ],
            compiler_params=pltpu.CompilerParams(collective_id=1, has_side_effects=True,
                                                 vmem_limit_bytes=VMEM_LIMIT - 2 * tokens * hidden_size - 65536),
            name='combine_scatter',
        )(expert_out, peer_out, heads, sides, hidden, shared_out)

    token_spec = P(('dp', 'ep'), None)
    expert_spec = P('ep', None, None)
    return jax.shard_map(
        local_step,
        mesh=mesh,
        in_specs=(token_spec, P(None), P(None, None), token_spec, expert_spec, expert_spec, expert_spec,
                  P(None, None), P(None, None), P(None, None)),
        out_specs=token_spec,
        check_vma=False,
    )
```

```python
import functools

import jax
import jax.numpy as jnp
from jax import lax
from jax.experimental import pallas as pl
from jax.experimental.pallas import tpu as pltpu
from jax.sharding import PartitionSpec as P

NORM_EPS = 1e-6
CORES = 2
VMEM_LIMIT = 67043328
F32 = jnp.float32
BF16 = jnp.bfloat16


def slots_of(side, first_expert, local_count, before):
    ids, weights = side[0:8], side[8:16]
    chosen, picked = [], []
    for e in range(8):
        hit = ids == (first_expert + e).astype(F32)
        chosen.append(jnp.sum(jnp.where(hit, 1.0, 0.0), axis=0, keepdims=True))
        picked.append(jnp.sum(jnp.where(hit, weights, 0.0), axis=0, keepdims=True))
    chosen = jnp.concatenate(chosen, axis=0)
    rank = jnp.dot(chosen.astype(BF16), before, preferred_element_type=F32)
    slot = jnp.where(chosen > 0.5, rank, -1000.0)
    return [slot[e:e + 1] for e in range(local_count)], picked[:local_count]


def place_of(group_size):
    chips = group_size // CORES
    me = lax.axis_index('ep')
    chip, core = me // CORES, me % CORES
    right = (chip + 1) % chips * CORES + core
    left = (chip + chips - 1) % chips * CORES + core
    return me, chip, core, right, left, chip * CORES + (1 - core)


def announce(neighbours):
    for device in neighbours:
        pl.semaphore_signal(pltpu.get_barrier_semaphore(), inc=1, device_id={'ep': device},
                            device_id_type=pl.DeviceIdType.MESH)


def meet(neighbours):
    pl.semaphore_wait(pltpu.get_barrier_semaphore(), len(neighbours))


def fill_before(before):
    row = lax.broadcasted_iota(jnp.int32, before.shape, 0)
    col = lax.broadcasted_iota(jnp.int32, before.shape, 1)
    before[...] = jnp.where(row < col, 1.0, 0.0).astype(BF16)


def remote(src, dst, send_sem, recv_sem, device):
    return pltpu.make_async_remote_copy(src_ref=src, dst_ref=dst, send_sem=send_sem, recv_sem=recv_sem,
                                        device_id={'ep': device}, device_id_type=pl.DeviceIdType.MESH)


def gather_kernel(group_size, capacity, slots, hidden_hbm, gain_hbm, router_hbm, idx_hbm,
                  sgate, sup, sdown, wgate, wup, wdown,
                  out_hbm, peer_hbm, head_hbm, side_hbm, shared_hbm,
                  gain_ref, router_ref, idx_ref, shared_ref, before_ref, rows, sides, x_ref, pick, gate_buf, up_buf, down_buf,
                  ring_s, ring_r, part_s, part_r, tring_s, tring_r, tpart_s, tpart_r, own_s, own_r,
                  head_s, head_r, peer_s, peer_r, load_sem, w_sem, out_sem):
    me, _, core, right, left, partner = place_of(group_size)
    local_count, hidden_size, ff = wgate.shape
    tokens = hidden_hbm.shape[0]
    half = tokens // 2
    half_cols = hidden_size // 2
    last = group_size // CORES - 1
    mine = pl.multiple_of(core * tokens, tokens)
    other = pl.multiple_of((1 - core) * tokens, tokens)

    def order(way, n):
        return min(2 * n + 1 + way, last)

    def piece(way, i, base):
        r = i % 2 if way == 0 else 1 - i % 2
        return rows.at[order(way, i // 2), pl.ds(pl.multiple_of(base + r * half, half), half)]

    def ring(way, i):
        n = i // 2
        r = i % 2 if way == 0 else 1 - i % 2
        src = 0 if n == 0 else order(way, n - 1)
        return remote(rows.at[src, pl.ds(pl.multiple_of(mine + r * half, half), half)], piece(way, i, mine),
                      ring_s.at[way, i], ring_r.at[way, i], right if way == 0 else left)

    def part(way, i, base):
        return remote(piece(way, i, base), piece(way, i, base), part_s.at[way, i], part_r.at[way, i], partner)

    def tring(way, n):
        src = 0 if n == 0 else 2 * (n - 1) + 1 + way
        return remote(sides.at[src, core], sides.at[2 * n + 1 + way, core],
                      tring_s.at[way, n], tring_r.at[way, n], right if way == 0 else left)

    def tpart(way, n, who):
        place = sides.at[2 * n + 1 + way, who]
        return remote(place, place, tpart_s.at[way, n], tpart_r.at[way, n], partner)

    def own_part(base):
        place = rows.at[0, pl.ds(base, tokens)]
        return remote(place, place, own_s.at[0], own_r.at[0], partner)

    def own_tpart(who):
        place = sides.at[0, who]
        return remote(place, place, own_s.at[1], own_r.at[1], partner)

    sends = 7

    def send(i):
        for way in range(2):
            ring(way, i).start()
            if i % 2 == 0 and i > 0:
                tring(way, i // 2).start()

    def service(i):
        for way in range(2):
            ring(way, i).wait_recv()
            if i % 2 == 0:
                tring(way, i // 2).wait_recv()
        if i + 2 < sends:
            send(i + 2)
        for way in range(2):
            part(way, i, mine).start()
            if i % 2 == 0:
                tpart(way, i // 2, core).start()

    def partner_arrived(i):
        for way in range(2):
            part(way, i, other).wait_recv()
            if i % 2 == 0:
                tpart(way, i // 2, 1 - core).wait_recv()

    beside = (right - core, left - core)

    def head(way, step, e, cc, source):
        chip_row, cols = (((2, 0), (1, 1)), ((2, 1), (0, 0)))[way][step]
        return remote(x_ref.at[e, chip_row, pl.ds(cc * HEAD_START, HEAD_ROWS), cols * half_cols:(cols + 1) * half_cols],
                      head_hbm.at[way, step, source, e], head_s.at[way, step, e, cc], head_r.at[way, step, e, source],
                      beside[way] + cc)

    def send_heads(step, e):
        for way in range(2):
            for cc in range(CORES):
                head(way, step, e, cc, core).start()

    def peer(turn, first, count, e):
        return remote(x_ref.at[e, 0:count], peer_hbm.at[e, pl.ds(first, count)], peer_s.at[turn, e], peer_r.at[turn, e], partner)

    loads = (pltpu.make_async_copy(hidden_hbm, rows.at[0, pl.ds(mine, tokens)], load_sem.at[0]),
             pltpu.make_async_copy(gain_hbm, gain_ref, load_sem.at[1]),
             pltpu.make_async_copy(router_hbm, router_ref, load_sem.at[2]),
             pltpu.make_async_copy(idx_hbm, idx_ref, load_sem.at[3]))
    for copy in loads:
        copy.start()
    store_shared = pltpu.make_async_copy(shared_ref, shared_hbm, load_sem.at[4])
    store_side = pltpu.make_async_copy(sides.at[0:group_size // CORES], side_hbm, load_sem.at[5])

    def normalise(r):
        block = 32

        def one(i, carry):
            place = pl.ds(pl.multiple_of(mine + r * half + i * block, block), block)
            x = rows[0, place, :].astype(F32)
            inv_rms = lax.rsqrt(jnp.mean(x * x, axis=-1, keepdims=True) + NORM_EPS)
            rows[0, place, :] = (x * inv_rms * gain_ref[...]).astype(BF16)
            return carry
        lax.fori_loop(0, half // block, one, 0)

    def route():
        x = rows[0, pl.ds(mine, tokens), :]
        logits = lax.dot_general(router_ref[...], x, (((1,), (1,)), ((), ())), preferred_element_type=F32)
        top = jnp.exp(logits - jnp.max(logits, axis=0, keepdims=True))
        probs = top / jnp.sum(top, axis=0, keepdims=True)
        experts_id = lax.broadcasted_iota(jnp.int32, probs.shape, 0)
        sides[0, core] = jnp.full((16, tokens), -1.0, F32)
        for j in range(idx_ref.shape[0]):
            idx = idx_ref[j:j + 1, :]
            sides[0, core, j:j + 1, :] = idx.astype(F32)
            sides[0, core, 8 + j:9 + j, :] = jnp.sum(jnp.where(experts_id == idx, probs, 0.0), axis=0, keepdims=True)

    def gate_copies(slot, gate, up):
        return (pltpu.make_async_copy(gate, gate_buf.at[slot], w_sem.at[slot]),
                pltpu.make_async_copy(up, up_buf.at[slot], w_sem.at[2 + slot]))

    def start_gate(slot, gate, up):
        for copy in gate_copies(slot, gate, up):
            copy.start()

    def down_copy(slot, down):
        return pltpu.make_async_copy(down, down_buf.at[slot], w_sem.at[4 + slot])

    def shared_cols(ref, i):
        return ref.at[:, pl.ds(pl.multiple_of(i * ff, 128), ff)]

    neighbours = [device + cc for device in beside for cc in range(CORES)] + [partner]
    announce(neighbours)
    fill_before(before_ref)
    for copy in loads:
        copy.wait()
    start_gate(0, shared_cols(sgate, 0), shared_cols(sup, 0))
    down_copy(0, sdown.at[0:ff]).start()
    start_gate(1, shared_cols(sgate, 1), shared_cols(sup, 1))
    down_copy(1, sdown.at[ff:2 * ff]).start()
    normalise(0)
    meet(neighbours)
    ring(0, 0).start()
    normalise(1)
    ring(1, 0).start()
    send(1)
    own_part(mine).start()
    route()
    for way in range(2):
        tring(way, 0).start()
    own_tpart(core).start()

    def swiglu(x, slot, fresh, next_gate, next_down):
        if fresh:
            for copy in gate_copies(slot, wgate.at[0], wup.at[0]):
                copy.wait()
        gate_out = jnp.dot(x, gate_buf[slot], preferred_element_type=F32)
        up_out = jnp.dot(x, up_buf[slot], preferred_element_type=F32)
        act = (jax.nn.silu(gate_out) * up_out).astype(BF16)
        next_gate()
        if fresh:
            down_copy(slot, wdown.at[0]).wait()
        out = jnp.dot(act, down_buf[slot], preferred_element_type=F32)
        next_down()
        return out

    def nothing():
        pass

    shared_parts = 2

    def shared(i, carry):
        slot = i % 2

        shared_ref[...] += swiglu(rows[0, pl.ds(mine, tokens), :], slot, True,
                                  lambda: start_gate(slot, wgate.at[i], wup.at[i]), lambda: down_copy(slot, wdown.at[i]).start())
        return carry

    shared_ref[...] = jnp.zeros_like(shared_ref)
    lax.fori_loop(0, shared_parts, shared, 0)

    def dispatch(base, start, count):
        def one(ch, carry):
            for cc in range(CORES):
                slot, _ = slots_of(sides[ch, cc], me * local_count, local_count, before_ref[...])
                row_id = lax.broadcasted_iota(jnp.int32, (slots, tokens), 0).astype(F32)
                for e in range(local_count):
                    hit = row_id == slot[e] + float(capacity * cc)
                    pick[e * slots:(e + 1) * slots, cc * tokens:(cc + 1) * tokens] = jnp.where(hit, 1.0, 0.0).astype(BF16)
            step = min(512, hidden_size)
            for n in range(0, hidden_size, step):
                got = jnp.dot(pick[...], rows[ch, :, n:n + step], preferred_element_type=F32).astype(BF16)
                for e in range(local_count):
                    x_ref[e, ch - base, :, n:n + step] = got[e * slots:(e + 1) * slots]
            return carry
        lax.fori_loop(start, start + count, one, 0)

    def stage_copy(e, first, count):
        return pltpu.make_async_copy(x_ref.at[e, 0:count], out_hbm.at[e, pl.ds(first, count)], out_sem.at[e])

    def mlp(e, slot, begin, count, fresh, next_gate, next_down):
        x = x_ref[e, begin:begin + count].reshape(count * slots, hidden_size)
        out = swiglu(x, slot, fresh, next_gate, next_down).astype(BF16)
        x_ref[e, begin:begin + count] = out.reshape(count, slots, hidden_size)

    def gate_after(e, slot):
        ahead = (e + 2) % local_count
        start_gate(slot, wgate.at[ahead], wup.at[ahead])

    def down_after(e, slot):
        down_copy(slot, wdown.at[(e + 2) % local_count]).start()

    def put(turn, first, count, e):
        stage_copy(e, first, count).start()
        peer(turn, first, count, e).start()

    def experts(turn, first, count, middle):
        def one(e, carry):
            @pl.when(e == local_count // 2)
            def _():
                service(middle)
            mlp(e, e % 2, 0, count, True, lambda: gate_after(e, e % 2), lambda: down_after(e, e % 2))
            put(turn, first, count, e)
            return carry
        lax.fori_loop(0, local_count, one, 0)

    def last_experts(turn, first, count):
        def near(e, carry):
            mlp(e, e % 2, 0, count - 1, True, nothing, nothing)
            send_heads(1, e)
            return carry

        def far(e, carry):
            mlp(e, e % 2, count - 1, 1, False, lambda: gate_after(e, e % 2), lambda: down_after(e, e % 2))
            send_heads(0, e)
            put(turn, first, count, e)
            return carry

        def both(e, carry):
            mlp(e, e % 2, 0, count, True, nothing, nothing)
            send_heads(1, e)
            send_heads(0, e)
            put(turn, first, count, e)
            return carry

        lax.fori_loop(0, 2, near, 0)
        service(6)
        partner_arrived(6)
        dispatch(first, first + count - 1, 1)
        lax.fori_loop(0, 2, far, 0)
        lax.fori_loop(2, local_count, both, 0)

    def finish(turn, first, count):
        for e in range(local_count):
            stage_copy(e, first, count).wait()
            peer(turn, first, count, e).wait_send()

    service(0)
    own_part(other).wait_recv()
    own_tpart(1 - core).wait_recv()
    dispatch(0, 0, 1)
    store_shared.start()
    service(1)
    partner_arrived(0)
    partner_arrived(1)
    dispatch(0, 1, 2)
    experts(0, 0, 3, 2)
    service(3)
    finish(0, 0, 3)
    partner_arrived(2)
    partner_arrived(3)
    dispatch(3, 3, 2)
    experts(1, 3, 2, 4)
    service(5)
    finish(1, 3, 2)
    partner_arrived(4)
    partner_arrived(5)
    dispatch(5, 5, 2)
    last_experts(2, 5, 3)
    finish(2, 5, 3)
    store_side.start()
    for way in range(2):
        for i in range(sends):
            ring(way, i).wait_send()
            part(way, i, mine).wait_send()
            if i % 2 == 0:
                tring(way, i // 2).wait_send()
                tpart(way, i // 2, core).wait_send()
    own_part(mine).wait_send()
    own_tpart(core).wait_send()
    for turn, (first, count) in enumerate(((0, 3), (3, 2), (5, 3))):
        for e in range(local_count):
            peer(turn, first, count, e).wait_recv()
    store_shared.wait()
    store_side.wait()

    def settle(e, carry):
        for step in range(2):
            for way in range(2):
                for cc in range(CORES):
                    head(way, step, e, cc, cc).wait_recv()
                    head(way, step, e, cc, cc).wait_send()
        return carry
    lax.fori_loop(0, local_count, settle, 0)


def scatter_kernel(group_size, capacity, rows_hbm, peer_hbm, head_hbm, side_hbm, hidden_hbm, shared_hbm, out_ref,
                   side_ref, before_ref, hidden_ref, shared_ref, rows, heads, acc, ring_in, load_sem, head_sem, base_sem, ring_s, ring_r):
    _, chip, core, right, left, _ = place_of(group_size)
    _, local_count, chips, _, hidden_size = rows.shape
    tokens = hidden_ref.shape[0]
    half = hidden_size // 2
    last = chips - 1
    steps = 5
    window = pl.ds(pl.multiple_of(core * HEAD_START, HEAD_START), WINDOW)

    def load(ch):
        return (pltpu.make_async_copy(rows_hbm.at[:, ch, window], rows.at[core, :, ch], load_sem.at[0, ch]),
                pltpu.make_async_copy(peer_hbm.at[:, ch, window], rows.at[1 - core, :, ch], load_sem.at[1, ch]))

    def load_head(way, i):
        return pltpu.make_async_copy(head_hbm.at[way, i], heads.at[way, i, :, :, 0:HEAD_ROWS], head_sem.at[way, i])

    neighbours = (right, left)
    announce(neighbours)
    load_side = pltpu.make_async_copy(side_hbm, side_ref, base_sem.at[2])
    load_side.start()
    def start_loads(i):
        for way in range(2):
            load_head(way, i).start()
            for copy in load((last - 1, last - 2, 4, 3)[2 * i + way]):
                copy.start()

    load_base = (pltpu.make_async_copy(hidden_hbm, hidden_ref, base_sem.at[0]),
                 pltpu.make_async_copy(shared_hbm, shared_ref, base_sem.at[1]))
    start_loads(0)
    fill_before(before_ref)
    heads[:, :, :, :, HEAD_ROWS:WINDOW, :] = jnp.zeros((2, 2, CORES, local_count, WINDOW - HEAD_ROWS, half), BF16)

    def ring(way, i):
        return remote(acc.at[way, i % 2], ring_in.at[way, i], ring_s.at[way, i], ring_r.at[way, i],
                      right if way == 0 else left)

    def mix_of(ch, from_chip):
        count = CORES * local_count
        slot, weight = slots_of(side_ref[ch, core], from_chip * count, count, before_ref[...])
        row_id = lax.broadcasted_iota(jnp.int32, (WINDOW, tokens), 0).astype(F32)
        shift = (core * (capacity - HEAD_START)).astype(F32)
        return [jnp.where(row_id == slot[e] + shift, weight[e], 0.0) for e in range(count)]

    def unit(ch, h, way, i):
        col = pl.multiple_of(h * half, half)
        mix = mix_of(ch, chip)
        picked = [rows[cc, e, ch, :, pl.ds(col, half)] for cc in range(CORES) for e in range(local_count)]
        if i < 2:
            mix += mix_of(ch, (left + way * (right - left)) // CORES)
            picked += [heads[way, i, cc, e] for cc in range(CORES) for e in range(local_count)]
        mix = jnp.concatenate(mix, axis=0)
        picked = jnp.concatenate(picked, axis=0)
        high = mix.astype(BF16)
        rest = mix - high.astype(F32)
        mid = rest.astype(BF16)
        low = (rest - mid.astype(F32)).astype(BF16)
        total = jnp.dot(high.T, picked, preferred_element_type=F32)
        total += jnp.dot(mid.T, picked, preferred_element_type=F32)
        return total + jnp.dot(low.T, picked, preferred_element_type=F32)

    def units(i, chans, halves):
        def one(way, carry):
            ch = chans[0] + way * (chans[1] - chans[0])
            h = halves[0] + way * (halves[1] - halves[0])
            acc[way, i % 2] = unit(ch, h, way, i)
            return carry
        lax.fori_loop(0, 2, one, 0)

    load_side.wait()
    loaded = set()

    def ensure(ch):
        if ch not in loaded:
            loaded.add(ch)
            for copy in load(ch):
                copy.wait()

    for i in range(steps):
        k = 3 - (i + 1) // 2
        chans = (2 * k, 2 * k - 1)
        for ch in chans:
            ensure(ch)
        for way in range(2):
            if i < 2:
                load_head(way, i).wait()
            else:
                ring(way, i - 2).wait_send()
        if i == 0:
            start_loads(1)
            for ch in (2, 1, 0):
                for copy in load(ch):
                    copy.start()
            for copy in load_base:
                copy.start()
        units(i, chans, (i % 2, 1 - i % 2))
        if i == 0:
            meet(neighbours)
        for way in range(2):
            if i >= 2:
                ring(way, i - 2).wait_recv()
                acc[way, i % 2] = acc[way, i % 2] + ring_in[way, i - 2]
            ring(way, i).start()
    ensure(0)
    for way in range(2):
        ring(way, steps - 2).wait_send()
    units(steps, (0, 0), (0, 1))
    for copy in load_base:
        copy.wait()
    for h in range(2):
        ring(1 - h, steps - 2).wait_recv()
        cols = slice(h * half, (h + 1) * half)
        acc[h, steps % 2] = (acc[h, steps % 2] + ring_in[1 - h, steps - 2]
                             + shared_ref[:, cols] + hidden_ref[:, cols].astype(F32))
    for h in range(2):
        ring(h, steps - 1).wait_recv()
        cols = slice(h * half, (h + 1) * half)
        out_ref[:, cols] = (acc[h, steps % 2] + ring_in[h, steps - 1]).astype(BF16)
    for way in range(2):
        ring(way, steps - 1).wait_send()


WINDOW = 48
HEAD_START = 32
HEAD_ROWS = 40


def solution(mesh):
    group_size = mesh.shape['ep']
    chips = group_size // CORES

    def local_step(hidden, norm_gain, router_w, topk_idx, w_gate, w_up, w_down, shared_gate, shared_up, shared_down):
        tokens, hidden_size = hidden.shape
        num_experts = router_w.shape[1]
        local_count, _, ff = w_gate.shape
        capacity = 3 * tokens * topk_idx.shape[1] // (2 * num_experts)
        slots = (CORES * capacity + 15) // 16 * 16
        hbm = pl.BlockSpec(memory_space=pl.ANY)
        vmem = pl.BlockSpec(memory_space=pltpu.VMEM)
        dma = pltpu.SemaphoreType.DMA
        expert_out, peer_out, heads, sides, shared_out = pl.pallas_call(
            functools.partial(gather_kernel, group_size, capacity, slots),
            in_specs=[hbm] * 10,
            out_specs=(hbm,) * 5,
            out_shape=(jax.ShapeDtypeStruct((local_count, chips, slots, hidden_size), BF16),
                       jax.ShapeDtypeStruct((local_count, chips, slots, hidden_size), BF16),
                       jax.ShapeDtypeStruct((2, 2, CORES, local_count, HEAD_ROWS, hidden_size // 2), BF16),
                       jax.ShapeDtypeStruct((chips, CORES, 16, tokens), F32),
                       jax.ShapeDtypeStruct((tokens, hidden_size), F32)),
            scratch_shapes=[
                pltpu.VMEM((1, hidden_size), F32),
                pltpu.VMEM((num_experts, hidden_size), BF16),
                pltpu.VMEM((topk_idx.shape[1], tokens), jnp.int32),
                pltpu.VMEM((tokens, hidden_size), F32),
                pltpu.VMEM((tokens, tokens), BF16),
                pltpu.VMEM((chips, CORES * tokens, hidden_size), BF16),
                pltpu.VMEM((chips + 1, CORES, 16, tokens), F32),
                pltpu.VMEM((local_count, 3, slots, hidden_size), BF16),
                pltpu.VMEM((local_count * slots, CORES * tokens), BF16),
                pltpu.VMEM((2, hidden_size, ff), BF16),
                pltpu.VMEM((2, hidden_size, ff), BF16),
                pltpu.VMEM((2, ff, hidden_size), BF16),
                dma((2, 7)), dma((2, 7)), dma((2, 7)), dma((2, 7)),
                dma((2, 4)), dma((2, 4)), dma((2, 4)), dma((2, 4)),
                dma((2,)), dma((2,)), dma((2, 2, local_count, CORES)), dma((2, 2, local_count, CORES)),
                dma((3, local_count)), dma((3, local_count)),
                dma((6,)), dma((6,)), dma((local_count,)),
            ],
            compiler_params=pltpu.CompilerParams(collective_id=0, has_side_effects=True, vmem_limit_bytes=VMEM_LIMIT),
            name='gather_experts',
        )(hidden, norm_gain[None, :], router_w.T, topk_idx.T, shared_gate, shared_up, shared_down, w_gate, w_up, w_down)
        return pl.pallas_call(
            functools.partial(scatter_kernel, group_size, capacity),
            in_specs=[hbm] * 6,
            out_specs=vmem,
            out_shape=pltpu.VMEM((tokens, hidden_size), BF16),
            scratch_shapes=[
                pltpu.VMEM((chips, CORES, 16, tokens), F32),
                pltpu.VMEM((tokens, tokens), BF16),
                pltpu.VMEM((tokens, hidden_size), BF16),
                pltpu.VMEM((tokens, hidden_size), F32),
                pltpu.VMEM((CORES, local_count, chips, WINDOW, hidden_size), BF16),
                pltpu.VMEM((2, 2, CORES, local_count, WINDOW, hidden_size // 2), BF16),
                pltpu.VMEM((2, 2, tokens, hidden_size // 2), F32),
                pltpu.VMEM((2, 5, tokens, hidden_size // 2), F32),
                dma((CORES, chips)), dma((2, 2)), dma((3,)), dma((2, 5)), dma((2, 5)),
            ],
            compiler_params=pltpu.CompilerParams(collective_id=1, has_side_effects=True,
                                                 vmem_limit_bytes=VMEM_LIMIT - 2 * tokens * hidden_size - 65536),
            name='combine_scatter',
        )(expert_out, peer_out, heads, sides, hidden, shared_out)

    token_spec = P(('dp', 'ep'), None)
    expert_spec = P('ep', None, None)
    return jax.shard_map(
        local_step,
        mesh=mesh,
        in_specs=(token_spec, P(None), P(None, None), token_spec, expert_spec, expert_spec, expert_spec,
                  P(None, None), P(None, None), P(None, None)),
        out_specs=token_spec,
        check_vma=False,
    )
```
